32 devices in a mesh: zon: 8 (over z, y), mer: 4 (over x, core).
Axes of the slice: x: 2, y: 2, z: 4, core: 2. Of those that a mesh axis runs over, the one named last changes fastest.
Arguments:
- sea_level: float32 [512, 4096], P('mer', 'zon'), may hold values from -6 to 6
- forcing: float32 [512, 4096], P('mer', 'zon'), may hold values from -6 to 6
- link_weights: float32 [8, 512, 4096], P(None, 'mer', 'zon'), may hold values from 0.1 to 2
- excess: float32 [512, 4096], P('mer', 'zon'), may hold values from 0.05 to 0.5
- ocean_mask: int32 [512, 4096], P('mer', 'zon'), may hold values 0 or 1
- current: float32 [2, 512, 4096], P(None, 'mer', 'zon'), may hold values from -6 to 6
- intersection_block: int32 [32, 32, 32], P(('zon', 'mer')), may hold values from -1 to 511, as said below
- intersection_cols: int32 [32, 32, 32, 128], P(('zon', 'mer')), may hold values from -1 to 127, as said below
- ice_mass: float32 [32, 32, 32, 128], P(('zon', 'mer')), may hold values from 0.2 to 3
- coriolis: float32 [32, 32, 32, 128], P(('zon', 'mer')), may hold values from -1.5 to 1.5
- ice_start: float32 [2, 32, 32, 32, 128], P(None, ('zon', 'mer')), may hold values from -6 to 6
- wind_stress: float32 [2, 32, 32, 32, 128], P(None, ('zon', 'mer')), may hold values from -6 to 6
Outputs:
- surface: float32 [512, 4096], P('mer', 'zon')
- velocity: float32 [2, 32, 32, 32, 128], P(None, ('zon', 'mer'))
The draws below stay inside these ranges and needn't reach their ends.
Inputs may be any that keep to these rules, and one draw needn't show every extreme that they name: `intersection_block`: for each owner device and ice device, the live ocean block numbers come first among the 32 slots and empty slots hold -1; in every draw one ice device receives 32 live blocks from every owner device. `intersection_cols`: within a live intersection block the cells named by different rows are distinct; rows of empty slots are all -1.
All inputs are finite; a program needn't handle non-finite values. No bound on the sum of `ocean_mask` on one device may be relied on, other than what follows from the above.
Results may differ from the reference program's by a relative error of at most 0.00002.
Values sent between devices are 32-bit elements; how exact they have to be, the bound alone decides.
A program may use at most 256 MiB of HBM per device.

```python
import math
import jax
import jax.numpy as jnp
from jax import lax

LAT_DEV = 128
LON_DEV = 512
BLOCK = 128
SWEEPS = 2
ICE_SWEEPS = 3
NY = 512
NX = 4096
OCEAN_BLOCKS = 512
PAIR_SLOTS = 32
N_ZON = 8
N_MER = 4
DEVICES = 32


def intersection_lists(key):
    base = jax.random.fold_in(key, 7)
    subkeys = jax.random.split(base, 5)
    counts = jax.random.randint(subkeys[0], (DEVICES, DEVICES), 0, PAIR_SLOTS + 1)
    full_target = jax.random.randint(subkeys[1], (), 0, DEVICES)
    ice_index = jnp.arange(DEVICES)
    counts = jnp.where(ice_index[None, :] == full_target, PAIR_SLOTS, counts)
    empty_target = (full_target + 1) % DEVICES
    counts = counts.at[0, empty_target].set(0)
    slot_index = jnp.arange(PAIR_SLOTS)
    is_live = slot_index[None, None, :] < counts[:, :, None]
    chosen = jax.random.randint(subkeys[2], (DEVICES, DEVICES, PAIR_SLOTS), 0, OCEAN_BLOCKS)
    chosen = chosen.at[0, full_target, 0].set(OCEAN_BLOCKS - 1)
    blocks = jnp.where(is_live, chosen, -1)
    scores = jax.random.randint(subkeys[3], (DEVICES, DEVICES, PAIR_SLOTS, BLOCK), 0, 1 << 20) * BLOCK + jnp.arange(BLOCK)
    shuffled = jnp.argsort(scores, axis=-1).astype(jnp.int32)
    keep_row = jax.random.randint(subkeys[4], (DEVICES, DEVICES, PAIR_SLOTS, BLOCK), 0, 8) > 0
    columns = jnp.where(is_live[..., None] & keep_row, shuffled, -1)
    return (blocks.astype(jnp.int32), columns.astype(jnp.int32))


def draw_intersection_block(key, part):
    return intersection_lists(key)[0]


def draw_intersection_cols(key, part):
    return intersection_lists(key)[1]


def set_ends(entries, stream_key, low, top_value):
    longest = entries.shape.index(max(entries.shape))
    spots = []
    for shift in (0, 1):
        where = [jax.random.randint(jax.random.fold_in(stream_key, axis), (), 0, length) for axis, length in enumerate(entries.shape)]
        where[longest] = (where[longest] + shift) % entries.shape[longest]
        spots.append(tuple(where))
    return entries.at[spots[0]].set(low).at[spots[1]].set(top_value)


def block_scale(own_key, shape, cuts, smallest, high):
    gain = 1.0
    for axis_at, parts in cuts:
        steps = jax.random.uniform(jax.random.fold_in(jax.random.fold_in(own_key, 6), axis_at), (parts,), jnp.float32, smallest / len(cuts), high / len(cuts))
        gain = gain * jnp.repeat(jnp.exp(steps), shape[axis_at] // parts).reshape((-1,) + (1,) * (len(shape) - 1 - axis_at))
    return gain


def noise(stream_key, shape, deviation, limit, cuts=(), kind=jnp.bfloat16):
    array = deviation * jax.random.normal(stream_key, shape, jnp.float32)
    if cuts:
        array = array * block_scale(stream_key, shape, cuts, -0.22, 0.18)
    return jnp.clip(array, -limit, limit).astype(kind)


def setup_inputs(seed: int = 0) -> dict:
    splits = jax.random.split(jax.random.key(seed), 13)
    return {
        "sea_level": noise(splits[0], (NY, NX), 1.0, 6.0, ((0, 4), (1, 8)), jnp.float32),
        "forcing": noise(splits[1], (NY, NX), 1.0, 6.0, ((0, 4), (1, 8)), jnp.float32),
        "link_weights": jnp.clip(jnp.exp(math.log(2.0) - 2.9957323 * jax.random.uniform(splits[2], (8, NY, NX), jnp.float32) ** block_scale(splits[2], (8, NY, NX), ((1, 4), (2, 8)), -0.2, 0.2)), 0.1, 2.0),
        "excess": jnp.clip(jnp.exp(math.log(0.5) - 2.3025851 * jax.random.uniform(splits[3], (NY, NX), jnp.float32) ** block_scale(splits[3], (NY, NX), ((0, 4), (1, 8)), -0.2, 0.2)), 0.05, 0.5),
        "ocean_mask": set_ends((jax.random.randint(splits[4], (NY, NX), 0, 8) < 7).astype(jnp.int32), jax.random.fold_in(splits[4], 1), 0, 1),
        "current": noise(splits[5], (2, NY, NX), 1.0, 6.0, ((1, 4), (2, 8)), jnp.float32),
        "intersection_block": draw_intersection_block(jax.random.fold_in(splits[12], 71), 0),
        "intersection_cols": draw_intersection_cols(jax.random.fold_in(splits[12], 71), 0),
        "ice_mass": jnp.clip(jnp.exp(math.log(3.0) - 2.7080502 * jax.random.uniform(splits[8], (DEVICES, DEVICES, PAIR_SLOTS, BLOCK), jnp.float32) ** block_scale(splits[8], (DEVICES, DEVICES, PAIR_SLOTS, BLOCK), ((0, 32),), -0.2, 0.2)), 0.2, 3.0),
        "coriolis": jnp.clip(jax.random.uniform(splits[9], (DEVICES, DEVICES, PAIR_SLOTS, BLOCK), jnp.float32, -1.5, 1.5) * block_scale(splits[9], (DEVICES, DEVICES, PAIR_SLOTS, BLOCK), ((0, 32),), -0.4, 0.0), -1.5, 1.5),
        "ice_start": noise(splits[10], (2, DEVICES, DEVICES, PAIR_SLOTS, BLOCK), 1.0, 6.0, ((1, 32),), jnp.float32),
        "wind_stress": noise(splits[11], (2, DEVICES, DEVICES, PAIR_SLOTS, BLOCK), 1.0, 6.0, ((1, 32),), jnp.float32),
    }


drag_coeff = 1.0
link_coeff = 0.5
neighbour_steps = ((0, 1), (0, -1), (1, 0), (-1, 0), (1, 1), (1, -1), (-1, 1), (-1, -1))


def colour_sequence(sweep_count):
    return [0] + [1, 2, 3, 2, 1, 0] * sweep_count


def gauss_seidel(surface, source, link_weights, diagonal, is_ocean, pad_fn):
    row_count, col_count = surface.shape
    row_parity = lax.broadcasted_iota(jnp.int32, (row_count, col_count), 0) % 2
    col_parity = lax.broadcasted_iota(jnp.int32, (row_count, col_count), 1) % 2
    colours = 2 * row_parity + col_parity
    for colour in colour_sequence(SWEEPS):
        padded = pad_fn(surface)
        gathered = source
        for position, (row_step, col_step) in enumerate(neighbour_steps):
            gathered = gathered + link_weights[position] * padded[1 + row_step:1 + row_step + row_count, 1 + col_step:1 + col_step + col_count]
        surface = jnp.where(is_ocean & (colours == colour), gathered / diagonal, surface)
    return surface


def pad_whole(surface):
    wrapped = jnp.concatenate([surface[:, -1:], surface, surface[:, :1]], axis=1)
    return jnp.pad(wrapped, ((1, 1), (0, 0)))


def along_block(values):
    padded = jnp.pad(values, [(0, 0)] * (values.ndim - 1) + [(1, 1)])
    return padded[..., :-2] + padded[..., 2:]


def ice_momentum(ice_mass, coriolis, ice_start, wind_stress, current):
    diagonal = ice_mass + drag_coeff + 2.0 * link_coeff
    turning = coriolis * ice_mass
    determinant = diagonal * diagonal + turning * turning
    base_east = ice_mass * ice_start[0] + wind_stress[0] + drag_coeff * current[0]
    base_north = ice_mass * ice_start[1] + wind_stress[1] + drag_coeff * current[1]
    velocity = ice_start
    for sweep_index in range(ICE_SWEEPS):
        beside = along_block(velocity)
        right_east = base_east + link_coeff * beside[0]
        right_north = base_north + link_coeff * beside[1]
        velocity = jnp.stack([(diagonal * right_east + turning * right_north) / determinant,
                              (diagonal * right_north - turning * right_east) / determinant])
    return velocity


def reference(sea_level, forcing, link_weights, excess, ocean_mask, current, intersection_block, intersection_cols, ice_mass, coriolis, ice_start, wind_stress):
    blocks = current.reshape(2, N_MER, LAT_DEV, N_ZON, LON_DEV).transpose(0, 3, 1, 2, 4).reshape(2, DEVICES, OCEAN_BLOCKS, BLOCK)
    owners = jnp.arange(DEVICES, dtype=jnp.int32)[:, None, None]
    picked = blocks[:, owners, jnp.maximum(intersection_block, 0).astype(jnp.int32)]
    valid = intersection_cols >= 0
    values = jnp.take_along_axis(picked, jnp.maximum(intersection_cols, 0)[None], axis=4)
    values = jnp.where(valid[None], values, 0.0)
    ice_current = values.transpose(0, 2, 1, 3, 4)
    velocity = ice_momentum(ice_mass, coriolis, ice_start, wind_stress, ice_current)
    ice_drag = drag_coeff * (velocity - ice_current)
    owner_drag = ice_drag.transpose(2, 0, 1, 3, 4)
    target = jnp.where(valid, jnp.maximum(intersection_block, 0)[..., None] * BLOCK + intersection_cols, OCEAN_BLOCKS * BLOCK).astype(jnp.int32)

    def scatter_owner(pair):
        owner_target, owner_values = pair
        return jnp.zeros((2, OCEAN_BLOCKS * BLOCK), jnp.float32).at[:, owner_target.reshape(-1)].add(owner_values.reshape(2, -1), mode="drop")

    summed = lax.map(scatter_owner, (target, owner_drag))
    stress_grid = summed.reshape(N_ZON, N_MER, 2, LAT_DEV, LON_DEV).transpose(2, 1, 3, 0, 4).reshape(2, N_MER * LAT_DEV, N_ZON * LON_DEV)
    stress_north = stress_grid[1]
    zonal_diff = jnp.roll(stress_north, -1, axis=1) - jnp.roll(stress_north, 1, axis=1)
    padded_east = jnp.pad(stress_grid[0], ((1, 1), (0, 0)))
    meridional_diff = padded_east[2:] - padded_east[:-2]
    source = forcing + zonal_diff - meridional_diff
    is_ocean = ocean_mask > 0
    diagonal = jnp.where(is_ocean, (1.0 + excess) * jnp.sum(link_weights, axis=0), 1.0)
    surface = jnp.where(is_ocean, sea_level, 0.0)
    surface = gauss_seidel(surface, source, link_weights, diagonal, is_ocean, pad_whole)
    return surface, velocity
```

```python
import functools

import jax
import jax.numpy as jnp
from jax import lax
from jax.experimental import pallas as pl
from jax.experimental.pallas import tpu as pltpu
from jax.sharding import PartitionSpec as P

SWEEPS = 2
ICE_SWEEPS = 3
ROW_RIM = 8
COL_RIM = 16
LANES = 128

drag_coeff = 1.0
link_coeff = 0.5
VM = pl.BlockSpec(memory_space=pltpu.VMEM)
PARAMS = pltpu.CompilerParams(vmem_limit_bytes=48 * 1024 * 1024)


def cost(flops, nbytes):
    return pl.CostEstimate(flops=flops, bytes_accessed=nbytes, transcendentals=0)


def lane_take(values, index):
    return jnp.take_along_axis(values, index, axis=1, mode="promise_in_bounds")


def split3(values):
    high = values.astype(jnp.bfloat16)
    rest = values - high.astype(jnp.float32)
    middle = rest.astype(jnp.bfloat16)
    low = (rest - middle.astype(jnp.float32)).astype(jnp.bfloat16)
    return high, middle, low


def nn_dot(a, b):
    return lax.dot_general(a, b, (((1,), (0,)), ((), ())), preferred_element_type=jnp.float32)


def block_rows(blocks, tiles, rows):
    safe = jnp.maximum(blocks, 0)
    return jnp.where(blocks >= 0, (safe % tiles) * rows + safe // tiles, -1)


def gather_kernel(pairs, current_ref, blocks_ref, cols_ref, out_ref, parts):
    _, rows, width = current_ref.shape
    tiles = width // LANES
    for j in range(tiles):
        for c in range(2):
            for k, part in enumerate(split3(current_ref[c, :, j * LANES : (j + 1) * LANES])):
                parts[k, j * rows : (j + 1) * rows, c * LANES : (c + 1) * LANES] = part
    lane = lax.broadcasted_iota(jnp.int32, (LANES, LANES), 1)
    for g in range(blocks_ref.shape[0]):
        spread = jnp.broadcast_to(blocks_ref[g : g + 1, :], (LANES, LANES))
        turned = jnp.transpose(spread)
        pick = jnp.concatenate(
            [
                jnp.where(turned == lane + b * LANES, 1.0, 0.0).astype(jnp.bfloat16)
                for b in range(rows * tiles // LANES)
            ],
            axis=1,
        )
        picked = nn_dot(pick, parts[0]) + nn_dot(pick, parts[1]) + nn_dot(pick, parts[2])
        cols = cols_ref[g * LANES : (g + 1) * LANES, :]
        index = jnp.maximum(cols, 0)
        for c in range(2):
            taken = lane_take(picked[:, c * LANES : (c + 1) * LANES], index)
            taken = jnp.where(cols >= 0, taken, 0.0)
            for d in range(LANES // pairs):
                out_ref[g * (LANES // pairs) + d, c] = taken[d * pairs : (d + 1) * pairs]


def inverse_kernel(cols_ref, out_ref):
    lane = lax.broadcasted_iota(jnp.int32, (8, LANES), 1)
    sub = lax.broadcasted_iota(jnp.int32, (8, LANES), 0)
    order = (lane + 1).astype(jnp.float32)
    index = (lane % 16) * 8 + sub
    group = lane // 16

    def body(i, carry):
        at = pl.multiple_of(i * 8, 8)
        cols = cols_ref[pl.ds(at, 8), :]
        high = jnp.right_shift(cols, 4)
        low = jnp.bitwise_and(cols, 15)
        left = jnp.concatenate([jnp.where(high == h, 1.0, 0.0) for h in range(8)], axis=0)
        right = jnp.concatenate([jnp.where(low == b, order, 0.0) for b in range(16)], axis=0)
        product = lax.dot_general(
            left.astype(jnp.bfloat16),
            right.astype(jnp.bfloat16),
            (((1,), (1,)), ((), ())),
            preferred_element_type=jnp.float32,
        )
        found = jnp.zeros((8, LANES), jnp.float32)
        for h in range(8):
            found = jnp.where(group == h, lane_take(product[h * 8 : (h + 1) * 8], index), found)
        out_ref[pl.ds(at, 8), :] = found.astype(jnp.int32) - 1
        return carry

    lax.fori_loop(0, cols_ref.shape[0] // 8, body, 0, unroll=4)


def ice_kernel(mass_ref, coriolis_ref, start_ref, wind_ref, current_ref, velocity_ref, drag_ref):
    devices, pairs, width = mass_ref.shape
    lane = lax.broadcasted_iota(jnp.int32, (pairs, width), 1)
    first, last = lane == 0, lane == width - 1

    def beside(values):
        before = jnp.where(first, 0.0, pltpu.roll(values, 1, 1))
        after = jnp.where(last, 0.0, pltpu.roll(values, width - 1, 1))
        return before + after

    for d in range(devices):
        mass = mass_ref[d]
        diagonal = mass + drag_coeff + 2.0 * link_coeff
        turning = coriolis_ref[d] * mass
        inverse = 1.0 / (diagonal * diagonal + turning * turning)
        diagonal = diagonal * inverse
        turning = turning * inverse
        east, north = start_ref[0, d], start_ref[1, d]
        base_east = mass * east + wind_ref[0, d] + drag_coeff * current_ref[d, 0]
        base_north = mass * north + wind_ref[1, d] + drag_coeff * current_ref[d, 1]
        for _ in range(ICE_SWEEPS):
            right_east = base_east + link_coeff * beside(east)
            right_north = base_north + link_coeff * beside(north)
            east = diagonal * right_east + turning * right_north
            north = diagonal * right_north - turning * right_east
        velocity_ref[0, d] = east
        velocity_ref[1, d] = north
        drag_ref[d, 0] = drag_coeff * (east - current_ref[d, 0])
        drag_ref[d, 1] = drag_coeff * (north - current_ref[d, 1])


def scatter_kernel(pairs, drag_ref, blocks_ref, inverse_ref, out_ref, edge_ref, total):
    _, rows, width = out_ref.shape
    tiles = width // LANES
    count = rows * tiles
    row = lax.broadcasted_iota(jnp.int32, (count, LANES), 0)
    for g in range(blocks_ref.shape[0]):
        put = jnp.where(
            jnp.broadcast_to(blocks_ref[g : g + 1, :], (count, LANES)) == row, 1.0, 0.0
        ).astype(jnp.bfloat16)
        inverse = inverse_ref[g * LANES : (g + 1) * LANES, :]
        index = jnp.maximum(inverse, 0)
        halves = []
        for c in range(2):
            values = jnp.concatenate(
                [drag_ref[g * (LANES // pairs) + d, c] for d in range(LANES // pairs)], axis=0
            )
            halves.append(jnp.where(inverse >= 0, lane_take(values, index), 0.0))
        high, middle, low = split3(jnp.concatenate(halves, axis=1))
        added = nn_dot(put, high) + nn_dot(put, middle) + nn_dot(put, low)
        if g == 0:
            total[...] = added
        else:
            total[...] += added
    for c in range(2):
        for j in range(tiles):
            out_ref[c, :, j * LANES : (j + 1) * LANES] = total[
                j * rows : (j + 1) * rows, c * LANES : (c + 1) * LANES
            ]
    pack_edges([out_ref.at[0], out_ref.at[1]], edge_ref)


def pack_edges(refs, edge_ref):
    rows, width = refs[0].shape
    per = LANES // COL_RIM
    slot = lax.broadcasted_iota(jnp.int32, (rows, LANES), 1) // COL_RIM
    for start in range(0, len(refs), per):
        tile = start // per
        first = jnp.zeros((rows, LANES), jnp.float32)
        last = first
        for k, ref in enumerate(refs[start : start + per]):
            head = ref[:, :LANES]
            tail = ref[:, width - LANES :]
            if k:
                head = pltpu.roll(head, k * COL_RIM, 1)
            if (k + 1) * COL_RIM != LANES:
                tail = pltpu.roll(tail, (k + 1) * COL_RIM, 1)
            first = jnp.where(slot == k, head, first)
            last = jnp.where(slot == k, tail, last)
        edge_ref[0, :, tile * LANES : (tile + 1) * LANES] = first
        edge_ref[1, :, tile * LANES : (tile + 1) * LANES] = last


def prepare_kernel(sea_ref, forcing_ref, weights_ref, excess_ref, mask_ref, out_ref, edge_ref):
    total = weights_ref[0]
    for k in range(1, 8):
        total = total + weights_ref[k]
    ocean = mask_ref[...] > 0
    inverse = jnp.where(ocean, 1.0 / ((1.0 + excess_ref[...]) * total), 0.0)
    for k in range(8):
        out_ref[k] = weights_ref[k] * inverse
    out_ref[8] = inverse
    out_ref[9] = jnp.where(ocean, sea_ref[...], 0.0)
    out_ref[10] = forcing_ref[...]
    pack_edges([out_ref.at[k] for k in range(out_ref.shape[0])], edge_ref)


def widen_kernel(body_ref, east_ref, west_ref, tile_ref, rows_ref):
    arrays, rows, width = body_ref.shape
    per = LANES // COL_RIM
    slot = lax.broadcasted_iota(jnp.int32, (rows, LANES), 1) // COL_RIM
    for k in range(arrays):
        at = (k // per) * LANES
        spot = k % per
        east = east_ref[:, at : at + LANES]
        west = west_ref[:, at : at + LANES]
        if spot:
            east = pltpu.roll(east, LANES - spot * COL_RIM, 1)
        if spot != per - 1:
            west = pltpu.roll(west, LANES - (spot + 1) * COL_RIM, 1)
        tile_ref[k] = jnp.where(slot == 0, east, jnp.where(slot == per - 1, west, 0.0))
        for side, start in ((0, 0), (1, rows - ROW_RIM)):
            rows_ref[side, k, :, :width] = body_ref[k, start : start + ROW_RIM, :]
            rows_ref[side, k, :, width:] = tile_ref[k, start : start + ROW_RIM, :]


def sweep_kernel(
    body_ref, tile_ref, south_ref, north_ref,
    stress_ref, stress_tile_ref, stress_south_ref, stress_north_ref,
    out_ref, field, wide_ref, even_ref, odd_ref,
):
    arrays, rows, width = body_ref.shape
    tall, wide = rows + 2 * ROW_RIM, width + LANES
    half = tall // 2
    tiles = wide // LANES

    def gather_into(k, body, tile, south, north):
        for t in range(tiles):
            at = k * tiles + t
            part = slice(t * LANES, (t + 1) * LANES)
            field[at, :rows, :] = body[:, part] if t < tiles - 1 else tile[...]
            field[at, rows : rows + ROW_RIM, :] = south[:, part]
            field[at, rows + ROW_RIM :, :] = north[:, part]

    for k in range(arrays):
        gather_into(k, body_ref.at[k], tile_ref.at[k], south_ref.at[k], north_ref.at[k])
    for c in range(2):
        for ref, start, size, left, length in (
            (stress_ref, 0, rows, 0, width),
            (stress_tile_ref, 0, rows, width, LANES),
            (stress_south_ref, rows, ROW_RIM, 0, wide),
            (stress_north_ref, rows + ROW_RIM, ROW_RIM, 0, wide),
        ):
            wide_ref[c, start : start + size, left : left + length] = ref[c]
    east_stress = wide_ref[0]
    north_stress = wide_ref[1]
    change = (
        pltpu.roll(north_stress, wide - 1, 1)
        - pltpu.roll(north_stress, 1, 1)
        - pltpu.roll(east_stress, tall - 1, 0)
        + pltpu.roll(east_stress, 1, 0)
    )
    for t in range(tiles):
        part = change[:, t * LANES : (t + 1) * LANES]
        field[10 * tiles + t] = (field[10 * tiles + t] + part) * field[8 * tiles + t]

    even_rows, odd_rows = pl.ds(0, half, stride=2), pl.ds(1, half, stride=2)
    column_odd = lax.broadcasted_iota(jnp.int32, (half, wide), 1) % 2

    def take(k, which):
        return jnp.concatenate([field[k * tiles + t, which, :] for t in range(tiles)], axis=1)

    even_ref[...] = take(9, even_rows)
    odd_ref[...] = take(9, odd_rows)

    def phase(own_ref, other_ref, which, odd, colours):
        base = take(10, which)
        other = other_ref[...]
        if odd:
            above, below = other, pltpu.roll(other, half - 1, 0)
        else:
            above, below = pltpu.roll(other, 1, 0), other
        base = base + take(2, which) * below + take(3, which) * above
        base = base + take(4, which) * pltpu.roll(below, wide - 1, 1)
        base = base + take(5, which) * pltpu.roll(below, 1, 1)
        base = base + take(6, which) * pltpu.roll(above, wide - 1, 1)
        base = base + take(7, which) * pltpu.roll(above, 1, 1)
        own = own_ref[...]
        for parity in colours:
            new = base + take(0, which) * pltpu.roll(own, wide - 1, 1)
            new = new + take(1, which) * pltpu.roll(own, 1, 1)
            own = jnp.where(column_odd == parity, new, own)
        own_ref[...] = own

    runs = [(0, [0, 1])]
    for _ in range(SWEEPS):
        runs += [(1, [0, 1, 0]), (0, [1, 0, 1])]
    runs[-1] = (0, [1, 0])
    for odd, colours in runs:
        if odd:
            phase(odd_ref, even_ref, odd_rows, True, colours)
        else:
            phase(even_ref, odd_ref, even_rows, False, colours)
    for t in range(tiles - 1):
        part = slice(t * LANES, (t + 1) * LANES)
        field[t, pl.ds(0, rows // 2, stride=2), :] = even_ref[: rows // 2, part]
        field[t, pl.ds(1, rows // 2, stride=2), :] = odd_ref[: rows // 2, part]
        out_ref[:, part] = field[t, :rows, :]


def shift(values, axis, step, wrap):
    count = lax.axis_size(axis)
    pairs = [(i, (i + step) % count) for i in range(count) if wrap or 0 <= i + step < count]
    return lax.ppermute(values, axis, pairs)


def widen(body, edge):
    arrays, rows, width = body.shape
    east = shift(edge[0], "zon", -1, True)
    west = shift(edge[1], "zon", 1, True)
    tile, ends = pl.pallas_call(
        widen_kernel,
        out_shape=(
            jax.ShapeDtypeStruct((arrays, rows, LANES), jnp.float32),
            jax.ShapeDtypeStruct((2, arrays, ROW_RIM, width + LANES), jnp.float32),
        ),
        in_specs=[VM] * 3,
        out_specs=(VM, VM),
        compiler_params=PARAMS,
        cost_estimate=cost(arrays * rows * 1024, arrays * rows * 1024),
        name="widen",
    )(body, east, west)
    south = shift(ends[0], "mer", -1, False)
    north = shift(ends[1], "mer", 1, False)
    return tile, south, north


def local(
    sea_level,
    forcing,
    link_weights,
    excess,
    ocean_mask,
    current,
    intersection_block,
    intersection_cols,
    ice_mass,
    coriolis,
    ice_start,
    wind_stress,
):
    rows, width = sea_level.shape
    _, devices, pairs, block = intersection_cols.shape
    slots = devices * pairs
    tiles = width // LANES
    f32 = jnp.float32
    names = ("zon", "mer")
    blocks = block_rows(intersection_block.reshape(slots // LANES, LANES), tiles, rows)
    cols = intersection_cols.reshape(slots, block)
    ice_shape = (devices, pairs, block)
    slot_bytes = slots * block * 4

    values = pl.pallas_call(
        functools.partial(gather_kernel, pairs),
        out_shape=jax.ShapeDtypeStruct((devices, 2, pairs, block), f32),
        in_specs=[VM] * 3,
        out_specs=VM,
        scratch_shapes=[pltpu.VMEM((3, rows * tiles, 2 * LANES), jnp.bfloat16)],
        compiler_params=PARAMS,
        cost_estimate=cost(slots * rows * tiles * 1536, 4 * slot_bytes),
        name="pick",
    )(current, blocks, cols)
    ice_current = lax.all_to_all(values, names, split_axis=0, concat_axis=0, tiled=True)

    inverse = pl.pallas_call(
        inverse_kernel,
        out_shape=jax.ShapeDtypeStruct((slots, block), jnp.int32),
        in_specs=[VM],
        out_specs=VM,
        compiler_params=PARAMS,
        cost_estimate=cost(slots * block * 4096, 4 * slot_bytes),
        name="inverse",
    )(cols)
    arrays = 11
    edge_width = -(-arrays * COL_RIM // LANES) * LANES
    body, edge = pl.pallas_call(
        prepare_kernel,
        out_shape=(
            jax.ShapeDtypeStruct((arrays, rows, width), f32),
            jax.ShapeDtypeStruct((2, rows, edge_width), f32),
        ),
        in_specs=[VM] * 5,
        out_specs=(VM, VM),
        compiler_params=PARAMS,
        cost_estimate=cost(rows * width * 64, rows * width * 96),
        name="prepare",
    )(sea_level, forcing, link_weights, excess, ocean_mask)
    tile, south, north = widen(body, edge)

    steps = 4
    part = devices // steps
    one = pl.BlockSpec((part, pairs, block), lambda i: (i, 0, 0))
    two = pl.BlockSpec((2, part, pairs, block), lambda i: (0, i, 0, 0))
    turned = pl.BlockSpec((part, 2, pairs, block), lambda i: (i, 0, 0, 0))
    velocity, drag = pl.pallas_call(
        ice_kernel,
        grid=(steps,),
        out_shape=(
            jax.ShapeDtypeStruct((2,) + ice_shape, f32),
            jax.ShapeDtypeStruct((devices, 2, pairs, block), f32),
        ),
        in_specs=[one, one, two, two, turned],
        out_specs=(two, turned),
        compiler_params=PARAMS,
        cost_estimate=cost(slots * block * 80, 12 * slot_bytes),
        name="ice",
    )(
        ice_mass.reshape(ice_shape),
        coriolis.reshape(ice_shape),
        ice_start.reshape((2,) + ice_shape),
        wind_stress.reshape((2,) + ice_shape),
        ice_current,
    )
    returned = lax.all_to_all(drag, names, split_axis=0, concat_axis=0, tiled=True)

    stress, stress_edge = pl.pallas_call(
        functools.partial(scatter_kernel, pairs),
        out_shape=(
            jax.ShapeDtypeStruct((2, rows, width), f32),
            jax.ShapeDtypeStruct((2, rows, LANES), f32),
        ),
        in_specs=[VM] * 3,
        out_specs=(VM, VM),
        scratch_shapes=[pltpu.VMEM((rows * tiles, 2 * LANES), f32)],
        compiler_params=PARAMS,
        cost_estimate=cost(slots * rows * tiles * 1536, 4 * slot_bytes),
        name="put",
    )(returned, blocks, inverse)
    stress_tile, stress_south, stress_north = widen(stress, stress_edge)

    tall, wide = rows + 2 * ROW_RIM, width + LANES
    surface = pl.pallas_call(
        sweep_kernel,
        out_shape=jax.ShapeDtypeStruct((rows, width), f32),
        in_specs=[VM] * 8,
        out_specs=VM,
        scratch_shapes=[
            pltpu.VMEM((arrays * (wide // LANES), tall, LANES), f32),
            pltpu.VMEM((2, tall, wide), f32),
            pltpu.VMEM((tall // 2, wide), f32),
            pltpu.VMEM((tall // 2, wide), f32),
        ],
        compiler_params=PARAMS,
        cost_estimate=cost(rows * width * 200, rows * width * 64),
        name="sweep",
    )(body, tile, south, north, stress, stress_tile, stress_south, stress_north)
    return (surface, velocity.reshape((2, 1) + ice_shape))


def solution(mesh):
    return jax.shard_map(
        local,
        mesh=mesh,
        in_specs=(
            P("mer", "zon"),
            P("mer", "zon"),
            P(None, "mer", "zon"),
            P("mer", "zon"),
            P("mer", "zon"),
            P(None, "mer", "zon"),
            P(("zon", "mer"), None, None),
            P(("zon", "mer"), None, None, None),
            P(("zon", "mer"), None, None, None),
            P(("zon", "mer"), None, None, None),
            P(None, ("zon", "mer"), None, None, None),
            P(None, ("zon", "mer"), None, None, None),
        ),
        out_specs=(P("mer", "zon"), P(None, ("zon", "mer"), None, None, None)),
        check_vma=False,
    )
```

```python
import functools

import jax
import jax.numpy as jnp
from jax import lax
from jax.experimental import pallas as pl
from jax.experimental.pallas import tpu as pltpu
from jax.sharding import PartitionSpec as P

SWEEPS = 2
ICE_SWEEPS = 3
ROW_RIM = 8
COL_RIM = 16
LANES = 128

drag_coeff = 1.0
link_coeff = 0.5
VM = pl.BlockSpec(memory_space=pltpu.VMEM)
PARAMS = pltpu.CompilerParams(vmem_limit_bytes=48 * 1024 * 1024)


def cost(flops, nbytes):
    return pl.CostEstimate(flops=flops, bytes_accessed=nbytes, transcendentals=0)


def lane_take(values, index):
    return jnp.take_along_axis(values, index, axis=1, mode="promise_in_bounds")


def split3(values):
    high = values.astype(jnp.bfloat16)
    rest = values - high.astype(jnp.float32)
    middle = rest.astype(jnp.bfloat16)
    low = (rest - middle.astype(jnp.float32)).astype(jnp.bfloat16)
    return high, middle, low


def nn_dot(a, b):
    return lax.dot_general(a, b, (((1,), (0,)), ((), ())), preferred_element_type=jnp.float32)


def block_rows(blocks, tiles, rows):
    safe = jnp.maximum(blocks, 0)
    return jnp.where(blocks >= 0, (safe % tiles) * rows + safe // tiles, -1)


def gather_kernel(pairs, current_ref, blocks_ref, cols_ref, out_ref, parts):
    _, rows, width = current_ref.shape
    tiles = width // LANES
    for j in range(tiles):
        for c in range(2):
            for k, part in enumerate(split3(current_ref[c, :, j * LANES : (j + 1) * LANES])):
                parts[k, j * rows : (j + 1) * rows, c * LANES : (c + 1) * LANES] = part
    lane = lax.broadcasted_iota(jnp.int32, (LANES, LANES), 1)
    for g in range(blocks_ref.shape[0]):
        spread = jnp.broadcast_to(blocks_ref[g : g + 1, :], (LANES, LANES))
        turned = jnp.transpose(spread)
        pick = jnp.concatenate(
            [
                jnp.where(turned == lane + b * LANES, 1.0, 0.0).astype(jnp.bfloat16)
                for b in range(rows * tiles // LANES)
            ],
            axis=1,
        )
        picked = nn_dot(pick, parts[0]) + nn_dot(pick, parts[1]) + nn_dot(pick, parts[2])
        cols = cols_ref[g * LANES : (g + 1) * LANES, :]
        index = jnp.maximum(cols, 0)
        for c in range(2):
            taken = lane_take(picked[:, c * LANES : (c + 1) * LANES], index)
            taken = jnp.where(cols >= 0, taken, 0.0)
            for d in range(LANES // pairs):
                out_ref[g * (LANES // pairs) + d, c] = taken[d * pairs : (d + 1) * pairs]


def inverse_kernel(cols_ref, out_ref, last, back_copy):
    lane = lax.broadcasted_iota(jnp.int32, (8, LANES), 1)
    sub = lax.broadcasted_iota(jnp.int32, (8, LANES), 0)
    order = (lane + 1).astype(jnp.float32)
    index = (lane % 16) * 8 + sub
    group = lane // 16

    def body(i, carry):
        at = pl.multiple_of(i * 8, 8)
        cols = cols_ref[pl.ds(at, 8), :]
        high = jnp.right_shift(cols, 4)
        low = jnp.bitwise_and(cols, 15)
        left = jnp.concatenate([jnp.where(high == h, 1.0, 0.0) for h in range(8)], axis=0)
        right = jnp.concatenate([jnp.where(low == b, order, 0.0) for b in range(16)], axis=0)
        product = lax.dot_general(
            left.astype(jnp.bfloat16),
            right.astype(jnp.bfloat16),
            (((1,), (1,)), ((), ())),
            preferred_element_type=jnp.float32,
        )
        found = jnp.zeros((8, LANES), jnp.float32)
        for h in range(8):
            found = jnp.where(group == h, lane_take(product[h * 8 : (h + 1) * 8], index), found)
        out_ref[pl.ds(at, 8), :] = found.astype(jnp.int32) - 1
        return carry

    lax.fori_loop(0, 1, body, 0)
    back_copy(last).start()
    lax.fori_loop(1, cols_ref.shape[0] // 8, body, 0)


def ice_block(mass, coriolis, start, wind, current):
    pairs, width = mass.shape
    lane = lax.broadcasted_iota(jnp.int32, (pairs, width), 1)
    first, last = lane == 0, lane == width - 1

    def beside(values):
        before = jnp.where(first, 0.0, pltpu.roll(values, 1, 1))
        after = jnp.where(last, 0.0, pltpu.roll(values, width - 1, 1))
        return before + after

    diagonal = mass + drag_coeff + 2.0 * link_coeff
    turning = coriolis * mass
    inverse = 1.0 / (diagonal * diagonal + turning * turning)
    diagonal = diagonal * inverse
    turning = turning * inverse
    east, north = start
    base_east = mass * east + wind[0] + drag_coeff * current[0]
    base_north = mass * north + wind[1] + drag_coeff * current[1]
    for _ in range(ICE_SWEEPS):
        right_east = base_east + link_coeff * beside(east)
        right_north = base_north + link_coeff * beside(north)
        east = diagonal * right_east + turning * right_north
        north = diagonal * right_north - turning * right_east
    return east, north


def around(sizes, body_ref, edge_ref, east_ref, west_ref, south_ref, north_ref, send, recv):
    rows = body_ref.shape[1]
    nz, nm = sizes
    z, m = lax.axis_index("zon"), lax.axis_index("mer")
    top, end = pl.ds(0, ROW_RIM), pl.ds(rows - ROW_RIM, ROW_RIM)
    whole, after, before = pl.ds(0, rows), pl.ds(rows, ROW_RIM), pl.ds(rows + ROW_RIM, ROW_RIM)
    moves = [
        (edge_ref.at[0], east_ref.at[whole], -1, 0),
        (edge_ref.at[1], west_ref.at[whole], 1, 0),
        (body_ref.at[:, top], south_ref, 0, -1),
        (body_ref.at[:, end], north_ref, 0, 1),
        (edge_ref.at[0, top], east_ref.at[after], -1, -1),
        (edge_ref.at[0, end], east_ref.at[before], -1, 1),
        (edge_ref.at[1, top], west_ref.at[after], 1, -1),
        (edge_ref.at[1, end], west_ref.at[before], 1, 1),
    ]
    return [
        pltpu.make_async_remote_copy(
            src_ref=source,
            dst_ref=target,
            send_sem=send.at[i],
            recv_sem=recv.at[i],
            device_id={"zon": lax.rem(z + dz + nz, nz), "mer": lax.rem(m + dm + nm, nm)},
            device_id_type=pl.DeviceIdType.MESH,
        )
        for i, (source, target, dz, dm) in enumerate(moves)
    ]


def travel_kernel(
    sizes,
    values_ref, mass_ref, coriolis_ref, start_ref, wind_ref,
    sea_ref, forcing_ref, weights_ref, excess_ref, mask_ref, cols_ref,
    velocity_ref, returned_ref, inverse_ref, body_ref, east_ref, west_ref, south_ref, north_ref,
    arrived, drag, edge, send_out, recv_out, send_back, recv_back, send_rim, recv_rim,
):
    nz, nm = sizes
    count = nz * nm
    z, m = lax.axis_index("zon"), lax.axis_index("mer")
    me = z * nm + m

    def offsets(k):
        i = k // nm
        return nz // 2 + ((i + 1) // 2) * (1 - 2 * (i % 2)), nm - 1 - k % nm

    def ahead(k):
        dz, dm = offsets(k)
        return lax.rem(z + dz, nz), lax.rem(m + dm, nm)

    def behind(k):
        dz, dm = offsets(k)
        return lax.rem(z - dz + nz, nz), lax.rem(m - dm + nm, nm)

    def out_copy(k):
        pz, pm = ahead(k)
        return pltpu.make_async_remote_copy(
            src_ref=values_ref.at[pz * nm + pm],
            dst_ref=arrived.at[me],
            send_sem=send_out.at[k],
            recv_sem=recv_out.at[k],
            device_id={"zon": pz, "mer": pm},
            device_id_type=pl.DeviceIdType.MESH,
        )

    def back_copy(k):
        pz, pm = behind(k)
        return pltpu.make_async_remote_copy(
            src_ref=drag.at[k],
            dst_ref=returned_ref.at[me],
            send_sem=send_back.at[k],
            recv_sem=recv_back.at[k],
            device_id={"zon": pz, "mer": pm},
            device_id_type=pl.DeviceIdType.MESH,
        )

    barrier = pltpu.get_barrier_semaphore()

    def greet(k, carry):
        pz, pm = ahead(k)
        pl.semaphore_signal(
            barrier,
            inc=1,
            device_id={"zon": pz, "mer": pm},
            device_id_type=pl.DeviceIdType.MESH,
        )
        return carry

    lax.fori_loop(0, count - 1, greet, 0)
    pl.semaphore_wait(barrier, count - 1)

    def launch(k, carry):
        out_copy(k).start()
        return carry

    lax.fori_loop(0, count - 1, launch, 0)

    prepare_kernel(sea_ref, forcing_ref, weights_ref, excess_ref, mask_ref, body_ref, edge)

    def ice(at, from_ref):
        current = (from_ref[at, 0], from_ref[at, 1])
        east, north = ice_block(
            mass_ref[at],
            coriolis_ref[at],
            (start_ref[0, at], start_ref[1, at]),
            (wind_ref[0, at], wind_ref[1, at]),
            current,
        )
        velocity_ref[0, at] = east
        velocity_ref[1, at] = north
        return drag_coeff * (east - current[0]), drag_coeff * (north - current[1])

    own_east, own_north = ice(me, values_ref)
    returned_ref[me, 0] = own_east
    returned_ref[me, 1] = own_north

    rim = around(
        sizes, body_ref, edge, east_ref, west_ref, south_ref, north_ref, send_rim, recv_rim
    )
    for copy in rim:
        copy.start()

    def step(k, carry):
        out_copy(k).wait_recv()
        pz, pm = behind(k)
        east, north = ice(pz * nm + pm, arrived)
        drag[k, 0] = east
        drag[k, 1] = north

        @pl.when(k > 0)
        def _():
            back_copy(k - 1).start()

        return carry

    lax.fori_loop(0, count - 1, step, 0)
    inverse_kernel(cols_ref, inverse_ref, count - 2, back_copy)

    def finish(k, carry):
        out_copy(k).wait_send()
        back_copy(k).wait()
        return carry

    lax.fori_loop(0, count - 1, finish, 0)
    for copy in rim:
        copy.wait()


def scatter_kernel(pairs, drag_ref, blocks_ref, inverse_ref, out_ref, edge_ref, total):
    _, rows, width = out_ref.shape
    tiles = width // LANES
    count = rows * tiles
    row = lax.broadcasted_iota(jnp.int32, (count, LANES), 0)
    for g in range(blocks_ref.shape[0]):
        put = jnp.where(
            jnp.broadcast_to(blocks_ref[g : g + 1, :], (count, LANES)) == row, 1.0, 0.0
        ).astype(jnp.bfloat16)
        inverse = inverse_ref[g * LANES : (g + 1) * LANES, :]
        index = jnp.maximum(inverse, 0)
        halves = []
        for c in range(2):
            values = jnp.concatenate(
                [drag_ref[g * (LANES // pairs) + d, c] for d in range(LANES // pairs)], axis=0
            )
            halves.append(jnp.where(inverse >= 0, lane_take(values, index), 0.0))
        high, middle, low = split3(jnp.concatenate(halves, axis=1))
        added = nn_dot(put, high) + nn_dot(put, middle) + nn_dot(put, low)
        if g == 0:
            total[...] = added
        else:
            total[...] += added
    for c in range(2):
        for j in range(tiles):
            out_ref[c, :, j * LANES : (j + 1) * LANES] = total[
                j * rows : (j + 1) * rows, c * LANES : (c + 1) * LANES
            ]
    pack_edges([out_ref.at[0], out_ref.at[1]], edge_ref)


def pack_edges(refs, edge_ref):
    rows, width = refs[0].shape
    per = LANES // COL_RIM
    slot = lax.broadcasted_iota(jnp.int32, (rows, LANES), 1) // COL_RIM
    for start in range(0, len(refs), per):
        tile = start // per
        first = jnp.zeros((rows, LANES), jnp.float32)
        last = first
        for k, ref in enumerate(refs[start : start + per]):
            head = ref[:, :LANES]
            tail = ref[:, width - LANES :]
            if k:
                head = pltpu.roll(head, k * COL_RIM, 1)
            if (k + 1) * COL_RIM != LANES:
                tail = pltpu.roll(tail, (k + 1) * COL_RIM, 1)
            first = jnp.where(slot == k, head, first)
            last = jnp.where(slot == k, tail, last)
        edge_ref[0, :, tile * LANES : (tile + 1) * LANES] = first
        edge_ref[1, :, tile * LANES : (tile + 1) * LANES] = last


def prepare_kernel(sea_ref, forcing_ref, weights_ref, excess_ref, mask_ref, out_ref, edge_ref):
    total = weights_ref[0]
    for k in range(1, 8):
        total = total + weights_ref[k]
    ocean = mask_ref[...] > 0
    inverse = jnp.where(ocean, 1.0 / ((1.0 + excess_ref[...]) * total), 0.0)
    for k in range(8):
        out_ref[k] = weights_ref[k] * inverse
    out_ref[8] = inverse
    out_ref[9] = jnp.where(ocean, sea_ref[...], 0.0)
    out_ref[10] = forcing_ref[...]
    pack_edges([out_ref.at[k] for k in range(out_ref.shape[0])], edge_ref)


def sweep_kernel(
    sizes,
    stress_ref, stress_edge_ref, body_ref, east_ref, west_ref, south_ref, north_ref,
    out_ref,
    field, wide_ref, even_ref, odd_ref, late_east, late_west, late_south, late_north, send, recv,
):
    arrays, rows, width = body_ref.shape
    tall, wide = rows + 2 * ROW_RIM, width + LANES
    half = tall // 2
    tiles = wide // LANES
    per = LANES // COL_RIM
    nz, nm = sizes
    z, m = lax.axis_index("zon"), lax.axis_index("mer")
    barrier = pltpu.get_barrier_semaphore()
    for dz in (-1, 0, 1):
        for dm in (-1, 0, 1):
            if dz or dm:
                pl.semaphore_signal(
                    barrier,
                    inc=1,
                    device_id={"zon": lax.rem(z + dz + nz, nz), "mer": lax.rem(m + dm + nm, nm)},
                    device_id_type=pl.DeviceIdType.MESH,
                )
    pl.semaphore_wait(barrier, 8)
    rim = around(
        sizes, stress_ref, stress_edge_ref, late_east, late_west, late_south, late_north, send, recv
    )
    for copy in rim:
        copy.start()

    row = lax.broadcasted_iota(jnp.int32, (tall, LANES), 0)
    slot = lax.broadcasted_iota(jnp.int32, (tall, LANES), 1) // COL_RIM
    lower = jnp.where(m == nm - 1, rows, rows + ROW_RIM)
    upper = jnp.where(m == 0, tall, rows + ROW_RIM)
    known = (row < lower) | ((row >= rows + ROW_RIM) & (row >= upper))
    has_south = m < nm - 1
    has_north = m > 0

    def side_tile(k, east_ref, west_ref):
        at = (k // per) * LANES
        spot = k % per
        east = east_ref[:, at : at + LANES]
        west = west_ref[:, at : at + LANES]
        if spot:
            east = pltpu.roll(east, LANES - spot * COL_RIM, 1)
        if spot != per - 1:
            west = pltpu.roll(west, LANES - (spot + 1) * COL_RIM, 1)
        both = jnp.where(slot == 0, east, jnp.where(slot == per - 1, west, 0.0))
        return jnp.where(known, both, 0.0)

    for k in range(arrays):
        for t in range(tiles - 1):
            at = k * tiles + t
            part = slice(t * LANES, (t + 1) * LANES)
            field[at, :rows, :] = body_ref[k, :, part]
            field[at, rows : rows + ROW_RIM, :] = jnp.where(has_south, south_ref[k, :, part], 0.0)
            field[at, rows + ROW_RIM :, :] = jnp.where(has_north, north_ref[k, :, part], 0.0)
        field[k * tiles + tiles - 1] = side_tile(k, east_ref, west_ref)
    for c in range(2):
        wide_ref[c, :rows, :width] = stress_ref[c]
    for copy in rim:
        copy.wait()
    for c in range(2):
        wide_ref[c, rows : rows + ROW_RIM, :width] = jnp.where(has_south, late_south[c], 0.0)
        wide_ref[c, rows + ROW_RIM :, :width] = jnp.where(has_north, late_north[c], 0.0)
        wide_ref[c, :, width:] = side_tile(c, late_east, late_west)
    east_stress = wide_ref[0]
    north_stress = wide_ref[1]
    change = (
        pltpu.roll(north_stress, wide - 1, 1)
        - pltpu.roll(north_stress, 1, 1)
        - pltpu.roll(east_stress, tall - 1, 0)
        + pltpu.roll(east_stress, 1, 0)
    )
    for t in range(tiles):
        part = change[:, t * LANES : (t + 1) * LANES]
        field[10 * tiles + t] = (field[10 * tiles + t] + part) * field[8 * tiles + t]

    even_rows, odd_rows = pl.ds(0, half, stride=2), pl.ds(1, half, stride=2)
    column_odd = lax.broadcasted_iota(jnp.int32, (half, wide), 1) % 2

    def take(k, which):
        return jnp.concatenate([field[k * tiles + t, which, :] for t in range(tiles)], axis=1)

    even_ref[...] = take(9, even_rows)
    odd_ref[...] = take(9, odd_rows)

    def phase(own_ref, other_ref, which, odd, colours):
        base = take(10, which)
        other = other_ref[...]
        if odd:
            above, below = other, pltpu.roll(other, half - 1, 0)
        else:
            above, below = pltpu.roll(other, 1, 0), other
        base = base + take(2, which) * below + take(3, which) * above
        base = base + take(4, which) * pltpu.roll(below, wide - 1, 1)
        base = base + take(5, which) * pltpu.roll(below, 1, 1)
        base = base + take(6, which) * pltpu.roll(above, wide - 1, 1)
        base = base + take(7, which) * pltpu.roll(above, 1, 1)
        own = own_ref[...]
        for parity in colours:
            new = base + take(0, which) * pltpu.roll(own, wide - 1, 1)
            new = new + take(1, which) * pltpu.roll(own, 1, 1)
            own = jnp.where(column_odd == parity, new, own)
        own_ref[...] = own

    runs = [(0, [0, 1])]
    for _ in range(SWEEPS):
        runs += [(1, [0, 1, 0]), (0, [1, 0, 1])]
    runs[-1] = (0, [1, 0])
    for odd, colours in runs:
        if odd:
            phase(odd_ref, even_ref, odd_rows, True, colours)
        else:
            phase(even_ref, odd_ref, even_rows, False, colours)
    for t in range(tiles - 1):
        part = slice(t * LANES, (t + 1) * LANES)
        field[t, pl.ds(0, rows // 2, stride=2), :] = even_ref[: rows // 2, part]
        field[t, pl.ds(1, rows // 2, stride=2), :] = odd_ref[: rows // 2, part]
        out_ref[:, part] = field[t, :rows, :]


def local(
    sea_level,
    forcing,
    link_weights,
    excess,
    ocean_mask,
    current,
    intersection_block,
    intersection_cols,
    ice_mass,
    coriolis,
    ice_start,
    wind_stress,
):
    rows, width = sea_level.shape
    _, devices, pairs, block = intersection_cols.shape
    slots = devices * pairs
    tiles = width // LANES
    f32 = jnp.float32
    blocks = block_rows(intersection_block.reshape(slots // LANES, LANES), tiles, rows)
    cols = intersection_cols.reshape(slots, block)
    ice_shape = (devices, pairs, block)
    slot_bytes = slots * block * 4

    values = pl.pallas_call(
        functools.partial(gather_kernel, pairs),
        out_shape=jax.ShapeDtypeStruct((devices, 2, pairs, block), f32),
        in_specs=[VM] * 3,
        out_specs=VM,
        scratch_shapes=[pltpu.VMEM((3, rows * tiles, 2 * LANES), jnp.bfloat16)],
        compiler_params=PARAMS,
        cost_estimate=cost(slots * rows * tiles * 1536, 4 * slot_bytes),
        name="pick",
    )(current, blocks, cols)
    sizes = (lax.axis_size("zon"), lax.axis_size("mer"))
    arrays = 11
    tall, wide = rows + 2 * ROW_RIM, width + LANES
    edge_width = -(-arrays * COL_RIM // LANES) * LANES
    dma = pltpu.SemaphoreType.DMA
    velocity, returned, inverse, body, east, west, south, north = pl.pallas_call(
        functools.partial(travel_kernel, sizes),
        out_shape=(
            jax.ShapeDtypeStruct((2,) + ice_shape, f32),
            jax.ShapeDtypeStruct((devices, 2, pairs, block), f32),
            jax.ShapeDtypeStruct((slots, block), jnp.int32),
            jax.ShapeDtypeStruct((arrays, rows, width), f32),
            jax.ShapeDtypeStruct((tall, edge_width), f32),
            jax.ShapeDtypeStruct((tall, edge_width), f32),
            jax.ShapeDtypeStruct((arrays, ROW_RIM, width), f32),
            jax.ShapeDtypeStruct((arrays, ROW_RIM, width), f32),
        ),
        in_specs=[VM] * 11,
        out_specs=(VM,) * 8,
        scratch_shapes=[
            pltpu.VMEM((devices, 2, pairs, block), f32),
            pltpu.VMEM((devices, 2, pairs, block), f32),
            pltpu.VMEM((2, rows, edge_width), f32),
            dma((devices,)),
            dma((devices,)),
            dma((devices,)),
            dma((devices,)),
            dma((8,)),
            dma((8,)),
        ],
        compiler_params=pltpu.CompilerParams(
            vmem_limit_bytes=48 * 1024 * 1024, collective_id=0, has_side_effects=True
        ),
        cost_estimate=cost(slots * block * 4096, 16 * slot_bytes),
        name="travel",
    )(
        values,
        ice_mass.reshape(ice_shape),
        coriolis.reshape(ice_shape),
        ice_start.reshape((2,) + ice_shape),
        wind_stress.reshape((2,) + ice_shape),
        sea_level,
        forcing,
        link_weights,
        excess,
        ocean_mask,
        cols,
    )

    stress, stress_edge = pl.pallas_call(
        functools.partial(scatter_kernel, pairs),
        out_shape=(
            jax.ShapeDtypeStruct((2, rows, width), f32),
            jax.ShapeDtypeStruct((2, rows, LANES), f32),
        ),
        in_specs=[VM] * 3,
        out_specs=(VM, VM),
        scratch_shapes=[pltpu.VMEM((rows * tiles, 2 * LANES), f32)],
        compiler_params=PARAMS,
        cost_estimate=cost(slots * rows * tiles * 1536, 4 * slot_bytes),
        name="put",
    )(returned, blocks, inverse)
    surface = pl.pallas_call(
        functools.partial(sweep_kernel, sizes),
        out_shape=jax.ShapeDtypeStruct((rows, width), f32),
        in_specs=[VM] * 7,
        out_specs=VM,
        scratch_shapes=[
            pltpu.VMEM((arrays * (wide // LANES), tall, LANES), f32),
            pltpu.VMEM((2, tall, wide), f32),
            pltpu.VMEM((tall // 2, wide), f32),
            pltpu.VMEM((tall // 2, wide), f32),
            pltpu.VMEM((tall, LANES), f32),
            pltpu.VMEM((tall, LANES), f32),
            pltpu.VMEM((2, ROW_RIM, width), f32),
            pltpu.VMEM((2, ROW_RIM, width), f32),
            dma((8,)),
            dma((8,)),
        ],
        compiler_params=pltpu.CompilerParams(
            vmem_limit_bytes=48 * 1024 * 1024, collective_id=1, has_side_effects=True
        ),
        cost_estimate=cost(rows * width * 200, rows * width * 64),
        name="sweep",
    )(stress, stress_edge, body, east, west, south, north)
    return (surface, velocity.reshape((2, 1) + ice_shape))


def solution(mesh):
    return jax.shard_map(
        local,
        mesh=mesh,
        in_specs=(
            P("mer", "zon"),
            P("mer", "zon"),
            P(None, "mer", "zon"),
            P("mer", "zon"),
            P("mer", "zon"),
            P(None, "mer", "zon"),
            P(("zon", "mer"), None, None),
            P(("zon", "mer"), None, None, None),
            P(("zon", "mer"), None, None, None),
            P(("zon", "mer"), None, None, None),
            P(None, ("zon", "mer"), None, None, None),
            P(None, ("zon", "mer"), None, None, None),
        ),
        out_specs=(P("mer", "zon"), P(None, ("zon", "mer"), None, None, None)),
        check_vma=False,
    )
```

```python
import functools

import jax
import jax.numpy as jnp
from jax import lax
from jax.experimental import pallas as pl
from jax.experimental.pallas import tpu as pltpu
from jax.sharding import PartitionSpec as P

SWEEPS = 2
ICE_SWEEPS = 3
ROW_RIM = 8
COL_RIM = 16
LANES = 128

drag_coeff = 1.0
link_coeff = 0.5
VM = pl.BlockSpec(memory_space=pltpu.VMEM)
PARAMS = pltpu.CompilerParams(vmem_limit_bytes=48 * 1024 * 1024)


def cost(flops, nbytes):
    return pl.CostEstimate(flops=flops, bytes_accessed=nbytes, transcendentals=0)


def lane_take(values, index):
    return jnp.take_along_axis(values, index, axis=1, mode="promise_in_bounds")


def split3(values):
    high = values.astype(jnp.bfloat16)
    rest = values - high.astype(jnp.float32)
    middle = rest.astype(jnp.bfloat16)
    low = (rest - middle.astype(jnp.float32)).astype(jnp.bfloat16)
    return high, middle, low


def nn_dot(a, b):
    return lax.dot_general(a, b, (((1,), (0,)), ((), ())), preferred_element_type=jnp.float32)


def block_rows(blocks, tiles, rows):
    safe = jnp.maximum(blocks, 0)
    return jnp.where(blocks >= 0, (safe % tiles) * rows + safe // tiles, -1)


def gather_kernel(pairs, current_ref, blocks_ref, cols_ref, out_ref, parts):
    _, rows, width = current_ref.shape
    tiles = width // LANES
    for j in range(tiles):
        for c in range(2):
            for k, part in enumerate(split3(current_ref[c, :, j * LANES : (j + 1) * LANES])):
                parts[k, j * rows : (j + 1) * rows, c * LANES : (c + 1) * LANES] = part
    lane = lax.broadcasted_iota(jnp.int32, (LANES, LANES), 1)
    for g in range(blocks_ref.shape[0]):
        spread = jnp.broadcast_to(blocks_ref[g : g + 1, :], (LANES, LANES))
        turned = jnp.transpose(spread)
        pick = jnp.concatenate(
            [
                jnp.where(turned == lane + b * LANES, 1.0, 0.0).astype(jnp.bfloat16)
                for b in range(rows * tiles // LANES)
            ],
            axis=1,
        )
        picked = nn_dot(pick, parts[0]) + nn_dot(pick, parts[1]) + nn_dot(pick, parts[2])
        cols = cols_ref[g * LANES : (g + 1) * LANES, :]
        index = jnp.maximum(cols, 0)
        for c in range(2):
            taken = lane_take(picked[:, c * LANES : (c + 1) * LANES], index)
            taken = jnp.where(cols >= 0, taken, 0.0)
            for d in range(LANES // pairs):
                out_ref[g * (LANES // pairs) + d, c] = taken[d * pairs : (d + 1) * pairs]


def inverse_rows(cols):
    lane = lax.broadcasted_iota(jnp.int32, (8, LANES), 1)
    sub = lax.broadcasted_iota(jnp.int32, (8, LANES), 0)
    order = (lane + 1).astype(jnp.float32)
    index = (lane % 16) * 8 + sub
    group = lane // 16
    high = jnp.right_shift(cols, 4)
    low = jnp.bitwise_and(cols, 15)
    left = jnp.concatenate([jnp.where(high == h, 1.0, 0.0) for h in range(8)], axis=0)
    right = jnp.concatenate([jnp.where(low == b, order, 0.0) for b in range(16)], axis=0)
    product = lax.dot_general(
        left.astype(jnp.bfloat16),
        right.astype(jnp.bfloat16),
        (((1,), (1,)), ((), ())),
        preferred_element_type=jnp.float32,
    )
    found = jnp.zeros((8, LANES), jnp.float32)
    for h in range(8):
        found = jnp.where(group == h, lane_take(product[h * 8 : (h + 1) * 8], index), found)
    return found.astype(jnp.int32) - 1


def ice_block(mass, coriolis, start, wind, current):
    pairs, width = mass.shape
    lane = lax.broadcasted_iota(jnp.int32, (pairs, width), 1)
    first, last = lane == 0, lane == width - 1

    def beside(values):
        before = jnp.where(first, 0.0, pltpu.roll(values, 1, 1))
        after = jnp.where(last, 0.0, pltpu.roll(values, width - 1, 1))
        return before + after

    diagonal = mass + drag_coeff + 2.0 * link_coeff
    turning = coriolis * mass
    inverse = 1.0 / (diagonal * diagonal + turning * turning)
    diagonal = diagonal * inverse
    turning = turning * inverse
    east, north = start
    base_east = mass * east + wind[0] + drag_coeff * current[0]
    base_north = mass * north + wind[1] + drag_coeff * current[1]
    for _ in range(ICE_SWEEPS):
        right_east = base_east + link_coeff * beside(east)
        right_north = base_north + link_coeff * beside(north)
        east = diagonal * right_east + turning * right_north
        north = diagonal * right_north - turning * right_east
    return east, north


def around(sizes, body_ref, edge_ref, east_ref, west_ref, south_ref, north_ref, send, recv):
    rows = body_ref.shape[1]
    nz, nm = sizes
    z, m = lax.axis_index("zon"), lax.axis_index("mer")
    top, end = pl.ds(0, ROW_RIM), pl.ds(rows - ROW_RIM, ROW_RIM)
    whole, after, before = pl.ds(0, rows), pl.ds(rows, ROW_RIM), pl.ds(rows + ROW_RIM, ROW_RIM)
    moves = [
        (edge_ref.at[0], east_ref.at[whole], -1, 0),
        (edge_ref.at[1], west_ref.at[whole], 1, 0),
        (body_ref.at[:, top], south_ref, 0, -1),
        (body_ref.at[:, end], north_ref, 0, 1),
        (edge_ref.at[0, top], east_ref.at[after], -1, -1),
        (edge_ref.at[0, end], east_ref.at[before], -1, 1),
        (edge_ref.at[1, top], west_ref.at[after], 1, -1),
        (edge_ref.at[1, end], west_ref.at[before], 1, 1),
    ]
    return [
        pltpu.make_async_remote_copy(
            src_ref=source,
            dst_ref=target,
            send_sem=send.at[i],
            recv_sem=recv.at[i],
            device_id={"zon": lax.rem(z + dz + nz, nz), "mer": lax.rem(m + dm + nm, nm)},
            device_id_type=pl.DeviceIdType.MESH,
        )
        for i, (source, target, dz, dm) in enumerate(moves)
    ]


def travel_kernel(
    sizes,
    values_ref, mass_ref, coriolis_ref, start_ref, wind_ref,
    sea_ref, forcing_ref, weights_ref, excess_ref, mask_ref, cols_ref,
    velocity_ref, returned_ref, inverse_ref, body_ref, east_ref, west_ref, south_ref, north_ref,
    arrived, drag, edge, send_out, recv_out, send_back, recv_back, send_rim, recv_rim,
):
    nz, nm = sizes
    count = nz * nm
    z, m = lax.axis_index("zon"), lax.axis_index("mer")
    me = z * nm + m

    def offsets(k):
        i = k // nm
        return nz // 2 + ((i + 1) // 2) * (1 - 2 * (i % 2)), nm - 1 - k % nm

    def ahead(k):
        dz, dm = offsets(k)
        return lax.rem(z + dz, nz), lax.rem(m + dm, nm)

    def behind(k):
        dz, dm = offsets(k)
        return lax.rem(z - dz + nz, nz), lax.rem(m - dm + nm, nm)

    def out_copy(k):
        pz, pm = ahead(k)
        return pltpu.make_async_remote_copy(
            src_ref=values_ref.at[pz * nm + pm],
            dst_ref=arrived.at[me],
            send_sem=send_out.at[k],
            recv_sem=recv_out.at[k],
            device_id={"zon": pz, "mer": pm},
            device_id_type=pl.DeviceIdType.MESH,
        )

    def back_copy(k):
        pz, pm = behind(k)
        return pltpu.make_async_remote_copy(
            src_ref=drag.at[k],
            dst_ref=returned_ref.at[me],
            send_sem=send_back.at[k],
            recv_sem=recv_back.at[k],
            device_id={"zon": pz, "mer": pm},
            device_id_type=pl.DeviceIdType.MESH,
        )

    barrier = pltpu.get_barrier_semaphore()

    def greet(k, carry):
        pz, pm = ahead(k)
        pl.semaphore_signal(
            barrier,
            inc=1,
            device_id={"zon": pz, "mer": pm},
            device_id_type=pl.DeviceIdType.MESH,
        )
        return carry

    lax.fori_loop(0, count - 1, greet, 0)
    pl.semaphore_wait(barrier, count - 1)

    def launch(k, carry):
        out_copy(k).start()
        return carry

    lax.fori_loop(0, count - 1, launch, 0)

    prepare_kernel(sea_ref, forcing_ref, weights_ref, excess_ref, mask_ref, body_ref, edge)

    def ice(at, from_ref):
        current = (from_ref[at, 0], from_ref[at, 1])
        east, north = ice_block(
            mass_ref[at],
            coriolis_ref[at],
            (start_ref[0, at], start_ref[1, at]),
            (wind_ref[0, at], wind_ref[1, at]),
            current,
        )
        velocity_ref[0, at] = east
        velocity_ref[1, at] = north
        return drag_coeff * (east - current[0]), drag_coeff * (north - current[1])

    pairs = mass_ref.shape[1]

    def invert(k):
        for r in range(0, pairs, 8):
            inverse_ref[k, r : r + 8] = inverse_rows(cols_ref[k, r : r + 8])

    own_east, own_north = ice(me, values_ref)
    invert(count - 1)
    returned_ref[me, 0] = own_east
    returned_ref[me, 1] = own_north

    rim = around(
        sizes, body_ref, edge, east_ref, west_ref, south_ref, north_ref, send_rim, recv_rim
    )
    for copy in rim:
        copy.start()

    def step(k, carry):
        out_copy(k).wait_recv()
        pz, pm = behind(k)
        east, north = ice(pz * nm + pm, arrived)
        drag[k, 0] = east
        drag[k, 1] = north
        invert(k)

        @pl.when(k > 0)
        def _():
            back_copy(k - 1).start()

        return carry

    lax.fori_loop(0, count - 1, step, 0)
    back_copy(count - 2).start()

    def finish(k, carry):
        out_copy(k).wait_send()
        back_copy(k).wait()
        return carry

    lax.fori_loop(0, count - 1, finish, 0)
    for copy in rim:
        copy.wait()


def scatter_kernel(pairs, drag_ref, blocks_ref, inverse_ref, out_ref, edge_ref, total):
    _, rows, width = out_ref.shape
    tiles = width // LANES
    count = rows * tiles
    row = lax.broadcasted_iota(jnp.int32, (count, LANES), 0)
    for g in range(blocks_ref.shape[0]):
        put = jnp.where(
            jnp.broadcast_to(blocks_ref[g : g + 1, :], (count, LANES)) == row, 1.0, 0.0
        ).astype(jnp.bfloat16)
        inverse = inverse_ref[g * LANES : (g + 1) * LANES, :]
        index = jnp.maximum(inverse, 0)
        halves = []
        for c in range(2):
            values = jnp.concatenate(
                [drag_ref[g * (LANES // pairs) + d, c] for d in range(LANES // pairs)], axis=0
            )
            halves.append(jnp.where(inverse >= 0, lane_take(values, index), 0.0))
        high, middle, low = split3(jnp.concatenate(halves, axis=1))
        added = nn_dot(put, high) + nn_dot(put, middle) + nn_dot(put, low)
        if g == 0:
            total[...] = added
        else:
            total[...] += added
    for c in range(2):
        for j in range(tiles):
            out_ref[c, :, j * LANES : (j + 1) * LANES] = total[
                j * rows : (j + 1) * rows, c * LANES : (c + 1) * LANES
            ]
    pack_edges([out_ref.at[0], out_ref.at[1]], edge_ref)


def pack_edges(refs, edge_ref):
    rows, width = refs[0].shape
    per = LANES // COL_RIM
    slot = lax.broadcasted_iota(jnp.int32, (rows, LANES), 1) // COL_RIM
    for start in range(0, len(refs), per):
        tile = start // per
        first = jnp.zeros((rows, LANES), jnp.float32)
        last = first
        for k, ref in enumerate(refs[start : start + per]):
            head = ref[:, :LANES]
            tail = ref[:, width - LANES :]
            if k:
                head = pltpu.roll(head, k * COL_RIM, 1)
            if (k + 1) * COL_RIM != LANES:
                tail = pltpu.roll(tail, (k + 1) * COL_RIM, 1)
            first = jnp.where(slot == k, head, first)
            last = jnp.where(slot == k, tail, last)
        edge_ref[0, :, tile * LANES : (tile + 1) * LANES] = first
        edge_ref[1, :, tile * LANES : (tile + 1) * LANES] = last


def prepare_kernel(sea_ref, forcing_ref, weights_ref, excess_ref, mask_ref, out_ref, edge_ref):
    total = weights_ref[0]
    for k in range(1, 8):
        total = total + weights_ref[k]
    ocean = mask_ref[...] > 0
    inverse = jnp.where(ocean, 1.0 / ((1.0 + excess_ref[...]) * total), 0.0)
    for k in range(8):
        out_ref[k] = weights_ref[k] * inverse
    out_ref[8] = inverse
    out_ref[9] = jnp.where(ocean, sea_ref[...], 0.0)
    out_ref[10] = forcing_ref[...]
    pack_edges([out_ref.at[k] for k in range(out_ref.shape[0])], edge_ref)


def sweep_kernel(
    sizes,
    stress_ref, stress_edge_ref, body_ref, east_ref, west_ref, south_ref, north_ref,
    out_ref,
    field, wide_ref, even_ref, odd_ref, late_east, late_west, late_south, late_north, send, recv,
):
    arrays, rows, width = body_ref.shape
    tall, wide = rows + 2 * ROW_RIM, width + LANES
    half = tall // 2
    tiles = wide // LANES
    per = LANES // COL_RIM
    nz, nm = sizes
    z, m = lax.axis_index("zon"), lax.axis_index("mer")
    barrier = pltpu.get_barrier_semaphore()
    for dz in (-1, 0, 1):
        for dm in (-1, 0, 1):
            if dz or dm:
                pl.semaphore_signal(
                    barrier,
                    inc=1,
                    device_id={"zon": lax.rem(z + dz + nz, nz), "mer": lax.rem(m + dm + nm, nm)},
                    device_id_type=pl.DeviceIdType.MESH,
                )
    pl.semaphore_wait(barrier, 8)
    rim = around(
        sizes, stress_ref, stress_edge_ref, late_east, late_west, late_south, late_north, send, recv
    )
    for copy in rim:
        copy.start()

    row = lax.broadcasted_iota(jnp.int32, (tall, LANES), 0)
    slot = lax.broadcasted_iota(jnp.int32, (tall, LANES), 1) // COL_RIM
    lower = jnp.where(m == nm - 1, rows, rows + ROW_RIM)
    upper = jnp.where(m == 0, tall, rows + ROW_RIM)
    known = (row < lower) | ((row >= rows + ROW_RIM) & (row >= upper))
    has_south = m < nm - 1
    has_north = m > 0

    def side_tile(k, east_ref, west_ref):
        at = (k // per) * LANES
        spot = k % per
        east = east_ref[:, at : at + LANES]
        west = west_ref[:, at : at + LANES]
        if spot:
            east = pltpu.roll(east, LANES - spot * COL_RIM, 1)
        if spot != per - 1:
            west = pltpu.roll(west, LANES - (spot + 1) * COL_RIM, 1)
        both = jnp.where(slot == 0, east, jnp.where(slot == per - 1, west, 0.0))
        return jnp.where(known, both, 0.0)

    for k in range(arrays):
        for t in range(tiles - 1):
            at = k * tiles + t
            part = slice(t * LANES, (t + 1) * LANES)
            field[at, :rows, :] = body_ref[k, :, part]
            field[at, rows : rows + ROW_RIM, :] = jnp.where(has_south, south_ref[k, :, part], 0.0)
            field[at, rows + ROW_RIM :, :] = jnp.where(has_north, north_ref[k, :, part], 0.0)
        field[k * tiles + tiles - 1] = side_tile(k, east_ref, west_ref)
    for c in range(2):
        wide_ref[c, :rows, :width] = stress_ref[c]
    for copy in rim:
        copy.wait()
    for c in range(2):
        wide_ref[c, rows : rows + ROW_RIM, :width] = jnp.where(has_south, late_south[c], 0.0)
        wide_ref[c, rows + ROW_RIM :, :width] = jnp.where(has_north, late_north[c], 0.0)
        wide_ref[c, :, width:] = side_tile(c, late_east, late_west)
    east_stress = wide_ref[0]
    north_stress = wide_ref[1]
    change = (
        pltpu.roll(north_stress, wide - 1, 1)
        - pltpu.roll(north_stress, 1, 1)
        - pltpu.roll(east_stress, tall - 1, 0)
        + pltpu.roll(east_stress, 1, 0)
    )
    for t in range(tiles):
        part = change[:, t * LANES : (t + 1) * LANES]
        field[10 * tiles + t] = (field[10 * tiles + t] + part) * field[8 * tiles + t]

    even_rows, odd_rows = pl.ds(0, half, stride=2), pl.ds(1, half, stride=2)
    column_odd = lax.broadcasted_iota(jnp.int32, (half, wide), 1) % 2

    def take(k, which):
        return jnp.concatenate([field[k * tiles + t, which, :] for t in range(tiles)], axis=1)

    even_ref[...] = take(9, even_rows)
    odd_ref[...] = take(9, odd_rows)

    def phase(own_ref, other_ref, which, odd, colours):
        base = take(10, which)
        other = other_ref[...]
        if odd:
            above, below = other, pltpu.roll(other, half - 1, 0)
        else:
            above, below = pltpu.roll(other, 1, 0), other
        base = base + take(2, which) * below + take(3, which) * above
        base = base + take(4, which) * pltpu.roll(below, wide - 1, 1)
        base = base + take(5, which) * pltpu.roll(below, 1, 1)
        base = base + take(6, which) * pltpu.roll(above, wide - 1, 1)
        base = base + take(7, which) * pltpu.roll(above, 1, 1)
        own = own_ref[...]
        for parity in colours:
            new = base + take(0, which) * pltpu.roll(own, wide - 1, 1)
            new = new + take(1, which) * pltpu.roll(own, 1, 1)
            own = jnp.where(column_odd == parity, new, own)
        own_ref[...] = own

    runs = [(0, [0, 1])]
    for _ in range(SWEEPS):
        runs += [(1, [0, 1, 0]), (0, [1, 0, 1])]
    runs[-1] = (0, [1, 0])
    for odd, colours in runs:
        if odd:
            phase(odd_ref, even_ref, odd_rows, True, colours)
        else:
            phase(even_ref, odd_ref, even_rows, False, colours)
    for t in range(tiles - 1):
        part = slice(t * LANES, (t + 1) * LANES)
        field[t, pl.ds(0, rows // 2, stride=2), :] = even_ref[: rows // 2, part]
        field[t, pl.ds(1, rows // 2, stride=2), :] = odd_ref[: rows // 2, part]
        out_ref[:, part] = field[t, :rows, :]


def local(
    sea_level,
    forcing,
    link_weights,
    excess,
    ocean_mask,
    current,
    intersection_block,
    intersection_cols,
    ice_mass,
    coriolis,
    ice_start,
    wind_stress,
):
    rows, width = sea_level.shape
    _, devices, pairs, block = intersection_cols.shape
    slots = devices * pairs
    tiles = width // LANES
    f32 = jnp.float32
    blocks = block_rows(intersection_block.reshape(slots // LANES, LANES), tiles, rows)
    cols = intersection_cols.reshape(slots, block)
    ice_shape = (devices, pairs, block)
    slot_bytes = slots * block * 4

    values = pl.pallas_call(
        functools.partial(gather_kernel, pairs),
        out_shape=jax.ShapeDtypeStruct((devices, 2, pairs, block), f32),
        in_specs=[VM] * 3,
        out_specs=VM,
        scratch_shapes=[pltpu.VMEM((3, rows * tiles, 2 * LANES), jnp.bfloat16)],
        compiler_params=PARAMS,
        cost_estimate=cost(slots * rows * tiles * 1536, 4 * slot_bytes),
        name="pick",
    )(current, blocks, cols)
    sizes = (lax.axis_size("zon"), lax.axis_size("mer"))
    arrays = 11
    tall, wide = rows + 2 * ROW_RIM, width + LANES
    edge_width = -(-arrays * COL_RIM // LANES) * LANES
    dma = pltpu.SemaphoreType.DMA
    velocity, returned, inverse, body, east, west, south, north = pl.pallas_call(
        functools.partial(travel_kernel, sizes),
        out_shape=(
            jax.ShapeDtypeStruct((2,) + ice_shape, f32),
            jax.ShapeDtypeStruct((devices, 2, pairs, block), f32),
            jax.ShapeDtypeStruct((devices, pairs, block), jnp.int32),
            jax.ShapeDtypeStruct((arrays, rows, width), f32),
            jax.ShapeDtypeStruct((tall, edge_width), f32),
            jax.ShapeDtypeStruct((tall, edge_width), f32),
            jax.ShapeDtypeStruct((arrays, ROW_RIM, width), f32),
            jax.ShapeDtypeStruct((arrays, ROW_RIM, width), f32),
        ),
        in_specs=[VM] * 11,
        out_specs=(VM,) * 8,
        scratch_shapes=[
            pltpu.VMEM((devices, 2, pairs, block), f32),
            pltpu.VMEM((devices, 2, pairs, block), f32),
            pltpu.VMEM((2, rows, edge_width), f32),
            dma((devices,)),
            dma((devices,)),
            dma((devices,)),
            dma((devices,)),
            dma((8,)),
            dma((8,)),
        ],
        compiler_params=pltpu.CompilerParams(
            vmem_limit_bytes=48 * 1024 * 1024, collective_id=0, has_side_effects=True
        ),
        cost_estimate=cost(slots * block * 4096, 16 * slot_bytes),
        name="travel",
    )(
        values,
        ice_mass.reshape(ice_shape),
        coriolis.reshape(ice_shape),
        ice_start.reshape((2,) + ice_shape),
        wind_stress.reshape((2,) + ice_shape),
        sea_level,
        forcing,
        link_weights,
        excess,
        ocean_mask,
        intersection_cols[0],
    )

    stress, stress_edge = pl.pallas_call(
        functools.partial(scatter_kernel, pairs),
        out_shape=(
            jax.ShapeDtypeStruct((2, rows, width), f32),
            jax.ShapeDtypeStruct((2, rows, LANES), f32),
        ),
        in_specs=[VM] * 3,
        out_specs=(VM, VM),
        scratch_shapes=[pltpu.VMEM((rows * tiles, 2 * LANES), f32)],
        compiler_params=PARAMS,
        cost_estimate=cost(slots * rows * tiles * 1536, 4 * slot_bytes),
        name="put",
    )(returned, blocks, inverse.reshape(slots, block))
    surface = pl.pallas_call(
        functools.partial(sweep_kernel, sizes),
        out_shape=jax.ShapeDtypeStruct((rows, width), f32),
        in_specs=[VM] * 7,
        out_specs=VM,
        scratch_shapes=[
            pltpu.VMEM((arrays * (wide // LANES), tall, LANES), f32),
            pltpu.VMEM((2, tall, wide), f32),
            pltpu.VMEM((tall // 2, wide), f32),
            pltpu.VMEM((tall // 2, wide), f32),
            pltpu.VMEM((tall, LANES), f32),
            pltpu.VMEM((tall, LANES), f32),
            pltpu.VMEM((2, ROW_RIM, width), f32),
            pltpu.VMEM((2, ROW_RIM, width), f32),
            dma((8,)),
            dma((8,)),
        ],
        compiler_params=pltpu.CompilerParams(
            vmem_limit_bytes=48 * 1024 * 1024, collective_id=1, has_side_effects=True
        ),
        cost_estimate=cost(rows * width * 200, rows * width * 64),
        name="sweep",
    )(stress, stress_edge, body, east, west, south, north)
    return (surface, velocity.reshape((2, 1) + ice_shape))


def solution(mesh):
    return jax.shard_map(
        local,
        mesh=mesh,
        in_specs=(
            P("mer", "zon"),
            P("mer", "zon"),
            P(None, "mer", "zon"),
            P("mer", "zon"),
            P("mer", "zon"),
            P(None, "mer", "zon"),
            P(("zon", "mer"), None, None),
            P(("zon", "mer"), None, None, None),
            P(("zon", "mer"), None, None, None),
            P(("zon", "mer"), None, None, None),
            P(None, ("zon", "mer"), None, None, None),
            P(None, ("zon", "mer"), None, None, None),
        ),
        out_specs=(P("mer", "zon"), P(None, ("zon", "mer"), None, None, None)),
        check_vma=False,
    )
```

```python
import functools

import jax
import jax.numpy as jnp
from jax import lax
from jax.experimental import pallas as pl
from jax.experimental.pallas import tpu as pltpu
from jax.sharding import PartitionSpec as P

SWEEPS = 2
ICE_SWEEPS = 3
ROW_RIM = 8
COL_RIM = 16
LANES = 128

drag_coeff = 1.0
link_coeff = 0.5
VM = pl.BlockSpec(memory_space=pltpu.VMEM)
HBM = pl.BlockSpec(memory_space=pltpu.HBM)
PARAMS = pltpu.CompilerParams(vmem_limit_bytes=48 * 1024 * 1024)


def cost(flops, nbytes):
    return pl.CostEstimate(flops=flops, bytes_accessed=nbytes, transcendentals=0)


def lane_take(values, index):
    return jnp.take_along_axis(values, index, axis=1, mode="promise_in_bounds")


def split3(values):
    high = values.astype(jnp.bfloat16)
    rest = values - high.astype(jnp.float32)
    middle = rest.astype(jnp.bfloat16)
    low = (rest - middle.astype(jnp.float32)).astype(jnp.bfloat16)
    return high, middle, low


def nn_dot(a, b):
    return lax.dot_general(a, b, (((1,), (0,)), ((), ())), preferred_element_type=jnp.float32)


def block_rows(blocks, tiles, rows):
    safe = jnp.maximum(blocks, 0)
    return jnp.where(blocks >= 0, (safe % tiles) * rows + safe // tiles, -1)


def gather_kernel(
    pairs, current_hbm, blocks_ref, cols_hbm, out_ref, parts, current_ref, cols_ref, loads
):
    _, rows, width = current_ref.shape
    tiles = width // LANES
    load_current = pltpu.make_async_copy(current_hbm, current_ref, loads.at[0])
    load_cols = pltpu.make_async_copy(cols_hbm, cols_ref, loads.at[1])
    load_current.start()
    load_cols.start()
    blocks = block_rows(blocks_ref[...], tiles, rows)
    load_current.wait()
    for j in range(tiles):
        for c in range(2):
            for k, part in enumerate(split3(current_ref[c, :, j * LANES : (j + 1) * LANES])):
                parts[k, j * rows : (j + 1) * rows, c * LANES : (c + 1) * LANES] = part
    lane = lax.broadcasted_iota(jnp.int32, (LANES, LANES), 1)
    load_cols.wait()
    for g in range(blocks_ref.shape[0]):
        spread = jnp.broadcast_to(blocks[g : g + 1, :], (LANES, LANES))
        turned = jnp.transpose(spread)
        pick = jnp.concatenate(
            [
                jnp.where(turned == lane + b * LANES, 1.0, 0.0).astype(jnp.bfloat16)
                for b in range(rows * tiles // LANES)
            ],
            axis=1,
        )
        picked = nn_dot(pick, parts[0]) + nn_dot(pick, parts[1]) + nn_dot(pick, parts[2])
        cols = cols_ref[g * LANES : (g + 1) * LANES, :]
        index = jnp.maximum(cols, 0)
        for c in range(2):
            taken = lane_take(picked[:, c * LANES : (c + 1) * LANES], index)
            taken = jnp.where(cols >= 0, taken, 0.0)
            for d in range(LANES // pairs):
                out_ref[g * (LANES // pairs) + d, c] = taken[d * pairs : (d + 1) * pairs]


def inverse_rows(cols):
    lane = lax.broadcasted_iota(jnp.int32, (8, LANES), 1)
    sub = lax.broadcasted_iota(jnp.int32, (8, LANES), 0)
    order = (lane + 1).astype(jnp.float32)
    index = (lane % 16) * 8 + sub
    group = lane // 16
    high = jnp.right_shift(cols, 4)
    low = jnp.bitwise_and(cols, 15)
    left = jnp.concatenate([jnp.where(high == h, 1.0, 0.0) for h in range(8)], axis=0)
    right = jnp.concatenate([jnp.where(low == b, order, 0.0) for b in range(16)], axis=0)
    product = lax.dot_general(
        left.astype(jnp.bfloat16),
        right.astype(jnp.bfloat16),
        (((1,), (1,)), ((), ())),
        preferred_element_type=jnp.float32,
    )
    found = jnp.zeros((8, LANES), jnp.float32)
    for h in range(8):
        found = jnp.where(group == h, lane_take(product[h * 8 : (h + 1) * 8], index), found)
    return found.astype(jnp.int32) - 1


def ice_block(mass, coriolis, start, wind, current):
    pairs, width = mass.shape
    lane = lax.broadcasted_iota(jnp.int32, (pairs, width), 1)
    first, last = lane == 0, lane == width - 1

    def beside(values):
        before = jnp.where(first, 0.0, pltpu.roll(values, 1, 1))
        after = jnp.where(last, 0.0, pltpu.roll(values, width - 1, 1))
        return before + after

    diagonal = mass + drag_coeff + 2.0 * link_coeff
    turning = coriolis * mass
    inverse = 1.0 / (diagonal * diagonal + turning * turning)
    diagonal = diagonal * inverse
    turning = turning * inverse
    east, north = start
    base_east = mass * east + wind[0] + drag_coeff * current[0]
    base_north = mass * north + wind[1] + drag_coeff * current[1]
    for _ in range(ICE_SWEEPS):
        right_east = base_east + link_coeff * beside(east)
        right_north = base_north + link_coeff * beside(north)
        east = diagonal * right_east + turning * right_north
        north = diagonal * right_north - turning * right_east
    return east, north


def around(sizes, body_ref, edge_ref, east_ref, west_ref, south_ref, north_ref, send, recv):
    rows = body_ref.shape[1]
    nz, nm = sizes
    z, m = lax.axis_index("zon"), lax.axis_index("mer")
    top, end = pl.ds(0, ROW_RIM), pl.ds(rows - ROW_RIM, ROW_RIM)
    whole, after, before = pl.ds(0, rows), pl.ds(rows, ROW_RIM), pl.ds(rows + ROW_RIM, ROW_RIM)
    moves = [
        (edge_ref.at[0], east_ref.at[whole], -1, 0),
        (edge_ref.at[1], west_ref.at[whole], 1, 0),
        (body_ref.at[:, top], south_ref, 0, -1),
        (body_ref.at[:, end], north_ref, 0, 1),
        (edge_ref.at[0, top], east_ref.at[after], -1, -1),
        (edge_ref.at[0, end], east_ref.at[before], -1, 1),
        (edge_ref.at[1, top], west_ref.at[after], 1, -1),
        (edge_ref.at[1, end], west_ref.at[before], 1, 1),
    ]
    return [
        pltpu.make_async_remote_copy(
            src_ref=source,
            dst_ref=target,
            send_sem=send.at[i],
            recv_sem=recv.at[i],
            device_id={"zon": lax.rem(z + dz + nz, nz), "mer": lax.rem(m + dm + nm, nm)},
            device_id_type=pl.DeviceIdType.MESH,
        )
        for i, (source, target, dz, dm) in enumerate(moves)
    ]


def travel_kernel(
    sizes,
    values_ref, mass_ref, coriolis_ref, start_ref, wind_ref,
    sea_ref, forcing_ref, weights_ref, excess_ref, mask_ref, cols_ref,
    velocity_ref, returned_ref, inverse_ref, body_ref, east_ref, west_ref, south_ref, north_ref,
    arrived, drag, edge, send_out, recv_out, send_back, recv_back, send_rim, recv_rim,
):
    nz, nm = sizes
    count = nz * nm
    z, m = lax.axis_index("zon"), lax.axis_index("mer")
    me = z * nm + m

    def offsets(k):
        i = k // nm
        return nz // 2 + ((i + 1) // 2) * (1 - 2 * (i % 2)), nm - 1 - k % nm

    def ahead(k):
        dz, dm = offsets(k)
        return lax.rem(z + dz, nz), lax.rem(m + dm, nm)

    def behind(k):
        dz, dm = offsets(k)
        return lax.rem(z - dz + nz, nz), lax.rem(m - dm + nm, nm)

    def out_copy(k):
        pz, pm = ahead(k)
        return pltpu.make_async_remote_copy(
            src_ref=values_ref.at[pz * nm + pm],
            dst_ref=arrived.at[me],
            send_sem=send_out.at[k],
            recv_sem=recv_out.at[k],
            device_id={"zon": pz, "mer": pm},
            device_id_type=pl.DeviceIdType.MESH,
        )

    def back_copy(k):
        pz, pm = behind(k)
        return pltpu.make_async_remote_copy(
            src_ref=drag.at[k],
            dst_ref=returned_ref.at[me],
            send_sem=send_back.at[k],
            recv_sem=recv_back.at[k],
            device_id={"zon": pz, "mer": pm},
            device_id_type=pl.DeviceIdType.MESH,
        )

    barrier = pltpu.get_barrier_semaphore()

    def greet(k, carry):
        pz, pm = ahead(k)
        pl.semaphore_signal(
            barrier,
            inc=1,
            device_id={"zon": pz, "mer": pm},
            device_id_type=pl.DeviceIdType.MESH,
        )
        return carry

    lax.fori_loop(0, count - 1, greet, 0)
    pl.semaphore_wait(barrier, count - 1)

    def launch(k, carry):
        out_copy(k).start()
        return carry

    lax.fori_loop(0, count - 1, launch, 0)

    prepare_kernel(sea_ref, forcing_ref, weights_ref, excess_ref, mask_ref, body_ref, edge)

    def ice(at, from_ref):
        current = (from_ref[at, 0], from_ref[at, 1])
        east, north = ice_block(
            mass_ref[at],
            coriolis_ref[at],
            (start_ref[0, at], start_ref[1, at]),
            (wind_ref[0, at], wind_ref[1, at]),
            current,
        )
        velocity_ref[0, at] = east
        velocity_ref[1, at] = north
        return drag_coeff * (east - current[0]), drag_coeff * (north - current[1])

    pairs = mass_ref.shape[1]

    def invert(k):
        for r in range(0, pairs, 8):
            inverse_ref[k, r : r + 8] = inverse_rows(cols_ref[k, r : r + 8])

    own_east, own_north = ice(me, values_ref)
    invert(count - 1)
    returned_ref[me, 0] = own_east
    returned_ref[me, 1] = own_north

    rim = around(
        sizes, body_ref, edge, east_ref, west_ref, south_ref, north_ref, send_rim, recv_rim
    )
    for copy in rim:
        copy.start()

    def step(k, carry):
        out_copy(k).wait_recv()
        pz, pm = behind(k)
        east, north = ice(pz * nm + pm, arrived)
        drag[k, 0] = east
        drag[k, 1] = north
        invert(k)

        @pl.when(k > 0)
        def _():
            back_copy(k - 1).start()

        return carry

    lax.fori_loop(0, count - 1, step, 0)
    back_copy(count - 2).start()

    def finish(k, carry):
        out_copy(k).wait_send()
        back_copy(k).wait()
        return carry

    lax.fori_loop(0, count - 1, finish, 0)
    for copy in rim:
        copy.wait()


def scatter_kernel(
    pairs, drag_ref, blocks_ref, inverse_ref, velocity_ref, out_ref, edge_ref, velocity_hbm,
    total, write,
):
    _, rows, width = out_ref.shape
    tiles = width // LANES
    count = rows * tiles
    write_velocity = pltpu.make_async_copy(velocity_ref, velocity_hbm, write)
    write_velocity.start()
    blocks = block_rows(blocks_ref[...], tiles, rows)
    row = lax.broadcasted_iota(jnp.int32, (count, LANES), 0)
    for g in range(blocks_ref.shape[0]):
        put = jnp.where(
            jnp.broadcast_to(blocks[g : g + 1, :], (count, LANES)) == row, 1.0, 0.0
        ).astype(jnp.bfloat16)
        inverse = inverse_ref[g * LANES : (g + 1) * LANES, :]
        index = jnp.maximum(inverse, 0)
        halves = []
        for c in range(2):
            values = jnp.concatenate(
                [drag_ref[g * (LANES // pairs) + d, c] for d in range(LANES // pairs)], axis=0
            )
            halves.append(jnp.where(inverse >= 0, lane_take(values, index), 0.0))
        high, middle, low = split3(jnp.concatenate(halves, axis=1))
        added = nn_dot(put, high) + nn_dot(put, middle) + nn_dot(put, low)
        if g == 0:
            total[...] = added
        else:
            total[...] += added
    for c in range(2):
        for j in range(tiles):
            out_ref[c, :, j * LANES : (j + 1) * LANES] = total[
                j * rows : (j + 1) * rows, c * LANES : (c + 1) * LANES
            ]
    pack_edges([out_ref.at[0], out_ref.at[1]], edge_ref)
    write_velocity.wait()


def pack_edges(refs, edge_ref):
    rows, width = refs[0].shape
    per = LANES // COL_RIM
    slot = lax.broadcasted_iota(jnp.int32, (rows, LANES), 1) // COL_RIM
    for start in range(0, len(refs), per):
        tile = start // per
        first = jnp.zeros((rows, LANES), jnp.float32)
        last = first
        for k, ref in enumerate(refs[start : start + per]):
            head = ref[:, :LANES]
            tail = ref[:, width - LANES :]
            if k:
                head = pltpu.roll(head, k * COL_RIM, 1)
            if (k + 1) * COL_RIM != LANES:
                tail = pltpu.roll(tail, (k + 1) * COL_RIM, 1)
            first = jnp.where(slot == k, head, first)
            last = jnp.where(slot == k, tail, last)
        edge_ref[0, :, tile * LANES : (tile + 1) * LANES] = first
        edge_ref[1, :, tile * LANES : (tile + 1) * LANES] = last


def prepare_kernel(sea_ref, forcing_ref, weights_ref, excess_ref, mask_ref, out_ref, edge_ref):
    total = weights_ref[0]
    for k in range(1, 8):
        total = total + weights_ref[k]
    ocean = mask_ref[...] > 0
    inverse = jnp.where(ocean, 1.0 / ((1.0 + excess_ref[...]) * total), 0.0)
    for k in range(8):
        out_ref[k] = weights_ref[k] * inverse
    out_ref[8] = inverse
    out_ref[9] = jnp.where(ocean, sea_ref[...], 0.0)
    out_ref[10] = forcing_ref[...]
    pack_edges([out_ref.at[k] for k in range(out_ref.shape[0])], edge_ref)


def sweep_kernel(
    sizes,
    stress_ref, stress_edge_ref, body_ref, east_ref, west_ref, south_ref, north_ref,
    out_ref,
    field, wide_ref, even_ref, odd_ref, late_east, late_west, late_south, late_north, send, recv,
):
    arrays, rows, width = body_ref.shape
    tall, wide = rows + 2 * ROW_RIM, width + LANES
    half = tall // 2
    tiles = wide // LANES
    per = LANES // COL_RIM
    nz, nm = sizes
    z, m = lax.axis_index("zon"), lax.axis_index("mer")
    barrier = pltpu.get_barrier_semaphore()
    for dz in (-1, 0, 1):
        for dm in (-1, 0, 1):
            if dz or dm:
                pl.semaphore_signal(
                    barrier,
                    inc=1,
                    device_id={"zon": lax.rem(z + dz + nz, nz), "mer": lax.rem(m + dm + nm, nm)},
                    device_id_type=pl.DeviceIdType.MESH,
                )
    pl.semaphore_wait(barrier, 8)
    rim = around(
        sizes, stress_ref, stress_edge_ref, late_east, late_west, late_south, late_north, send, recv
    )
    for copy in rim:
        copy.start()

    row = lax.broadcasted_iota(jnp.int32, (tall, LANES), 0)
    slot = lax.broadcasted_iota(jnp.int32, (tall, LANES), 1) // COL_RIM
    lower = jnp.where(m == nm - 1, rows, rows + ROW_RIM)
    upper = jnp.where(m == 0, tall, rows + ROW_RIM)
    known = (row < lower) | ((row >= rows + ROW_RIM) & (row >= upper))
    has_south = m < nm - 1
    has_north = m > 0

    def side_tile(k, east_ref, west_ref):
        at = (k // per) * LANES
        spot = k % per
        east = east_ref[:, at : at + LANES]
        west = west_ref[:, at : at + LANES]
        if spot:
            east = pltpu.roll(east, LANES - spot * COL_RIM, 1)
        if spot != per - 1:
            west = pltpu.roll(west, LANES - (spot + 1) * COL_RIM, 1)
        both = jnp.where(slot == 0, east, jnp.where(slot == per - 1, west, 0.0))
        return jnp.where(known, both, 0.0)

    for k in range(arrays):
        for t in range(tiles - 1):
            at = k * tiles + t
            part = slice(t * LANES, (t + 1) * LANES)
            field[at, :rows, :] = body_ref[k, :, part]
            field[at, rows : rows + ROW_RIM, :] = jnp.where(has_south, south_ref[k, :, part], 0.0)
            field[at, rows + ROW_RIM :, :] = jnp.where(has_north, north_ref[k, :, part], 0.0)
        field[k * tiles + tiles - 1] = side_tile(k, east_ref, west_ref)
    for c in range(2):
        wide_ref[c, :rows, :width] = stress_ref[c]
    for copy in rim:
        copy.wait()
    for c in range(2):
        wide_ref[c, rows : rows + ROW_RIM, :width] = jnp.where(has_south, late_south[c], 0.0)
        wide_ref[c, rows + ROW_RIM :, :width] = jnp.where(has_north, late_north[c], 0.0)
        wide_ref[c, :, width:] = side_tile(c, late_east, late_west)
    east_stress = wide_ref[0]
    north_stress = wide_ref[1]
    change = (
        pltpu.roll(north_stress, wide - 1, 1)
        - pltpu.roll(north_stress, 1, 1)
        - pltpu.roll(east_stress, tall - 1, 0)
        + pltpu.roll(east_stress, 1, 0)
    )
    for t in range(tiles):
        part = change[:, t * LANES : (t + 1) * LANES]
        field[10 * tiles + t] = (field[10 * tiles + t] + part) * field[8 * tiles + t]

    even_rows, odd_rows = pl.ds(0, half, stride=2), pl.ds(1, half, stride=2)
    column_odd = lax.broadcasted_iota(jnp.int32, (half, wide), 1) % 2

    def take(k, which):
        return jnp.concatenate([field[k * tiles + t, which, :] for t in range(tiles)], axis=1)

    even_ref[...] = take(9, even_rows)
    odd_ref[...] = take(9, odd_rows)

    def phase(own_ref, other_ref, which, odd, colours):
        base = take(10, which)
        other = other_ref[...]
        if odd:
            above, below = other, pltpu.roll(other, half - 1, 0)
        else:
            above, below = pltpu.roll(other, 1, 0), other
        base = base + take(2, which) * below + take(3, which) * above
        base = base + take(4, which) * pltpu.roll(below, wide - 1, 1)
        base = base + take(5, which) * pltpu.roll(below, 1, 1)
        base = base + take(6, which) * pltpu.roll(above, wide - 1, 1)
        base = base + take(7, which) * pltpu.roll(above, 1, 1)
        own = own_ref[...]
        for parity in colours:
            new = base + take(0, which) * pltpu.roll(own, wide - 1, 1)
            new = new + take(1, which) * pltpu.roll(own, 1, 1)
            own = jnp.where(column_odd == parity, new, own)
        own_ref[...] = own

    runs = [(0, [0, 1])]
    for _ in range(SWEEPS):
        runs += [(1, [0, 1, 0]), (0, [1, 0, 1])]
    runs[-1] = (0, [1, 0])
    for odd, colours in runs:
        if odd:
            phase(odd_ref, even_ref, odd_rows, True, colours)
        else:
            phase(even_ref, odd_ref, even_rows, False, colours)
    for t in range(tiles - 1):
        part = slice(t * LANES, (t + 1) * LANES)
        field[t, pl.ds(0, rows // 2, stride=2), :] = even_ref[: rows // 2, part]
        field[t, pl.ds(1, rows // 2, stride=2), :] = odd_ref[: rows // 2, part]
        out_ref[:, part] = field[t, :rows, :]


def local(
    sea_level,
    forcing,
    link_weights,
    excess,
    ocean_mask,
    current,
    intersection_block,
    intersection_cols,
    ice_mass,
    coriolis,
    ice_start,
    wind_stress,
):
    rows, width = sea_level.shape
    _, devices, pairs, block = intersection_cols.shape
    slots = devices * pairs
    tiles = width // LANES
    f32 = jnp.float32
    blocks = intersection_block.reshape(slots // LANES, LANES)
    cols = intersection_cols.reshape(slots, block)
    ice_shape = (devices, pairs, block)
    slot_bytes = slots * block * 4

    values = pl.pallas_call(
        functools.partial(gather_kernel, pairs),
        out_shape=jax.ShapeDtypeStruct((devices, 2, pairs, block), f32),
        in_specs=[HBM, VM, HBM],
        out_specs=VM,
        scratch_shapes=[
            pltpu.VMEM((3, rows * tiles, 2 * LANES), jnp.bfloat16),
            pltpu.VMEM((2, rows, width), f32),
            pltpu.VMEM((slots, block), jnp.int32),
            pltpu.SemaphoreType.DMA((2,)),
        ],
        compiler_params=PARAMS,
        cost_estimate=cost(slots * rows * tiles * 1536, 4 * slot_bytes),
        name="pick",
    )(current, blocks, cols)
    sizes = (lax.axis_size("zon"), lax.axis_size("mer"))
    arrays = 11
    tall, wide = rows + 2 * ROW_RIM, width + LANES
    edge_width = -(-arrays * COL_RIM // LANES) * LANES
    dma = pltpu.SemaphoreType.DMA
    velocity, returned, inverse, body, east, west, south, north = pl.pallas_call(
        functools.partial(travel_kernel, sizes),
        out_shape=(
            jax.ShapeDtypeStruct((2,) + ice_shape, f32),
            jax.ShapeDtypeStruct((devices, 2, pairs, block), f32),
            jax.ShapeDtypeStruct((devices, pairs, block), jnp.int32),
            jax.ShapeDtypeStruct((arrays, rows, width), f32),
            jax.ShapeDtypeStruct((tall, edge_width), f32),
            jax.ShapeDtypeStruct((tall, edge_width), f32),
            jax.ShapeDtypeStruct((arrays, ROW_RIM, width), f32),
            jax.ShapeDtypeStruct((arrays, ROW_RIM, width), f32),
        ),
        in_specs=[VM] * 11,
        out_specs=(VM,) * 8,
        scratch_shapes=[
            pltpu.VMEM((devices, 2, pairs, block), f32),
            pltpu.VMEM((devices, 2, pairs, block), f32),
            pltpu.VMEM((2, rows, edge_width), f32),
            dma((devices,)),
            dma((devices,)),
            dma((devices,)),
            dma((devices,)),
            dma((8,)),
            dma((8,)),
        ],
        compiler_params=pltpu.CompilerParams(
            vmem_limit_bytes=48 * 1024 * 1024, collective_id=0, has_side_effects=True
        ),
        cost_estimate=cost(slots * block * 4096, 16 * slot_bytes),
        name="travel",
    )(
        values,
        ice_mass.reshape(ice_shape),
        coriolis.reshape(ice_shape),
        ice_start.reshape((2,) + ice_shape),
        wind_stress.reshape((2,) + ice_shape),
        sea_level,
        forcing,
        link_weights,
        excess,
        ocean_mask,
        intersection_cols[0],
    )

    stress, stress_edge, velocity = pl.pallas_call(
        functools.partial(scatter_kernel, pairs),
        out_shape=(
            jax.ShapeDtypeStruct((2, rows, width), f32),
            jax.ShapeDtypeStruct((2, rows, LANES), f32),
            jax.ShapeDtypeStruct((2,) + ice_shape, f32),
        ),
        in_specs=[VM] * 4,
        out_specs=(VM, VM, HBM),
        scratch_shapes=[pltpu.VMEM((rows * tiles, 2 * LANES), f32), pltpu.SemaphoreType.DMA],
        compiler_params=PARAMS,
        cost_estimate=cost(slots * rows * tiles * 1536, 4 * slot_bytes),
        name="put",
    )(returned, blocks, inverse.reshape(slots, block), velocity)
    surface = pl.pallas_call(
        functools.partial(sweep_kernel, sizes),
        out_shape=jax.ShapeDtypeStruct((rows, width), f32),
        in_specs=[VM] * 7,
        out_specs=VM,
        scratch_shapes=[
            pltpu.VMEM((arrays * (wide // LANES), tall, LANES), f32),
            pltpu.VMEM((2, tall, wide), f32),
            pltpu.VMEM((tall // 2, wide), f32),
            pltpu.VMEM((tall // 2, wide), f32),
            pltpu.VMEM((tall, LANES), f32),
            pltpu.VMEM((tall, LANES), f32),
            pltpu.VMEM((2, ROW_RIM, width), f32),
            pltpu.VMEM((2, ROW_RIM, width), f32),
            dma((8,)),
            dma((8,)),
        ],
        compiler_params=pltpu.CompilerParams(
            vmem_limit_bytes=48 * 1024 * 1024, collective_id=1, has_side_effects=True
        ),
        cost_estimate=cost(rows * width * 200, rows * width * 64),
        name="sweep",
    )(stress, stress_edge, body, east, west, south, north)
    return (surface, velocity.reshape((2, 1) + ice_shape))


def solution(mesh):
    return jax.shard_map(
        local,
        mesh=mesh,
        in_specs=(
            P("mer", "zon"),
            P("mer", "zon"),
            P(None, "mer", "zon"),
            P("mer", "zon"),
            P("mer", "zon"),
            P(None, "mer", "zon"),
            P(("zon", "mer"), None, None),
            P(("zon", "mer"), None, None, None),
            P(("zon", "mer"), None, None, None),
            P(("zon", "mer"), None, None, None),
            P(None, ("zon", "mer"), None, None, None),
            P(None, ("zon", "mer"), None, None, None),
        ),
        out_specs=(P("mer", "zon"), P(None, ("zon", "mer"), None, None, None)),
        check_vma=False,
    )
```
